256 devices in a mesh: region: 16 (over z, core), feat: 16 (over y, x).
Axes of the slice: x: 4, y: 4, z: 8, core: 2. Of those that a mesh axis runs over, the one named last changes fastest.
Arguments:
- node_lat: bfloat16 [6144, 512], P(('region', 'feat')), may hold values from -6 to 6
- edge_lat: bfloat16 [49152, 512], P(('region', 'feat')), may hold values from -6 to 6
- receiver_row: int32 [49152], P('region'), may hold values from 0 to 383
- sender_slot: int32 [49152], P('region'), may hold values from 0 to 639, as said below
- send_rows: int32 [16, 16, 16], P('region'), may hold values from 0 to 383
- w_edge_in: bfloat16 [3, 512, 512], P(None, 'feat'), may hold values from -0.15625 to 0.15625
- w_edge_out: bfloat16 [512, 512], P('feat'), may hold values from -0.25 to 0.25
- w_node_in: bfloat16 [2, 512, 512], P(None, 'feat'), may hold values from -0.1875 to 0.1875
- w_node_out: bfloat16 [512, 512], P('feat'), may hold values from -0.25 to 0.25
- edge_gain: float32 [512], P('feat'), may hold values from 0.1 to 1.9
- node_gain: float32 [512], P('feat'), may hold values from 0.1 to 1.9
- node_cot: bfloat16 [6144, 512], P(('region', 'feat')), may hold values from -6 to 6
- edge_cot: bfloat16 [49152, 512], P(('region', 'feat')), may hold values from -6 to 6
Outputs:
- node_new: bfloat16 [6144, 512], P(('region', 'feat'))
- edge_new: bfloat16 [49152, 512], P(('region', 'feat'))
- node_grad: float32 [6144, 512], P(('region', 'feat'))
- edge_grad: float32 [49152, 512], P(('region', 'feat'))
- grad_edge_in: float32 [3, 512, 512], P(None, 'feat')
- grad_edge_out: float32 [512, 512], P('feat')
- grad_node_in: float32 [2, 512, 512], P(None, 'feat')
- grad_node_out: float32 [512, 512], P('feat')
The draws below stay inside these ranges and needn't reach their ends.
Inputs may be any that keep to these rules, and one draw needn't show every extreme that they name: `receiver_row`: edge e lies in region e // 3072; its receiver is that row of the region's 384 nodes. `sender_slot`: A value below 384 is a row of the edge's own region; a value 384 + p * 16 + s names the node that region p lists in slot s for the edge's region, and p is never the edge's own region. send_rows[p, r, s] is a row of region p's 384 nodes.
All inputs are finite; a program needn't handle non-finite values.
Results may differ from the reference program's by a relative error of at most 0.02.
Values may be sent and summed in bfloat16 or wider, within the bound.
A program may use at most 64 MiB of HBM per device.

```python
import jax
import jax.numpy as jnp
from jax import lax

D = 512
NODE_DEV = 384
DEGREE = 8
SLOTS = 16
REGIONS = 16
EDGE_DEV = 3072
NODES = 6144
EDGES = 49152


def draw_sender_slot(key, part):
    edge_total = NODE_DEV * DEGREE * REGIONS
    subkeys = jax.random.split(jax.random.fold_in(key, 17), 6)
    region = jnp.arange(edge_total, dtype=jnp.int32) // (NODE_DEV * DEGREE)
    kind_draw = jax.random.randint(subkeys[0], (edge_total,), 0, 10)
    local_rows = jax.random.randint(subkeys[1], (edge_total,), 0, NODE_DEV)
    near_steps = jax.random.randint(subkeys[2], (edge_total,), 1, 4) * (2 * jax.random.randint(subkeys[3], (edge_total,), 0, 2) - 1)
    far_steps = jax.random.randint(subkeys[4], (edge_total,), 1, REGIONS)
    step_draw = jnp.where(kind_draw < 7, near_steps, far_steps)
    peer_ids = (region + step_draw) % REGIONS
    slot_draw = jax.random.randint(subkeys[5], (edge_total,), 0, SLOTS)
    return jnp.where(kind_draw < 4, local_rows, NODE_DEV + peer_ids * SLOTS + slot_draw).astype(jnp.int32)


def set_ends(array, own_key, smallest, top_value):
    place = [jax.random.randint(jax.random.fold_in(own_key, axis), (), 0, length) for axis, length in enumerate(array.shape)]
    widest = array.shape.index(max(array.shape))
    neighbour = place[:widest] + [(place[widest] + 1) % array.shape[widest]] + place[widest + 1:]
    return array.at[tuple(place)].set(smallest).at[tuple(neighbour)].set(top_value)


def shard_levels(stream_key, extent, shards, low, high):
    level = 1.0
    for axis_at, parts in shards:
        heights = jax.random.uniform(jax.random.fold_in(jax.random.fold_in(stream_key, 6), axis_at), (parts,), jnp.float32, low / len(shards), high / len(shards))
        level = level * jnp.repeat(jnp.exp(heights), extent[axis_at] // parts).reshape((-1,) + (1,) * (len(extent) - 1 - axis_at))
    return level


def noise(own_key, extent, width, bound, shards=(), held_as=jnp.bfloat16):
    entries = width * jax.random.normal(own_key, extent, jnp.float32)
    if shards:
        entries = entries * shard_levels(own_key, extent, shards, -0.22, 0.18)
    return jnp.clip(entries, -bound, bound).astype(held_as)


def setup_inputs(seed: int = 0) -> dict:
    arg_keys = jax.random.split(jax.random.key(seed), 14)
    return {
        "node_lat": noise(arg_keys[0], (NODES, D), 1.0, 6.0, ((0, 256),)),
        "edge_lat": noise(arg_keys[1], (EDGES, D), 1.0, 6.0, ((0, 256),)),
        "receiver_row": set_ends(jax.random.randint(arg_keys[2], (EDGES,), 0, NODE_DEV), jax.random.fold_in(arg_keys[2], 1), 0, NODE_DEV - 1).astype(jnp.int32),
        "sender_slot": draw_sender_slot(jax.random.fold_in(arg_keys[13], 71), 0),
        "send_rows": set_ends(jax.random.randint(arg_keys[4], (REGIONS, REGIONS, SLOTS), 0, NODE_DEV), jax.random.fold_in(arg_keys[4], 1), 0, NODE_DEV - 1).astype(jnp.int32),
        "w_edge_in": noise(arg_keys[5], (3, D, D), (3 * D) ** -0.5, 0.15625, ((1, 16),)),
        "w_edge_out": noise(arg_keys[6], (D, D), D ** -0.5, 0.25, ((0, 16),)),
        "w_node_in": noise(arg_keys[7], (2, D, D), (2 * D) ** -0.5, 0.1875, ((1, 16),)),
        "w_node_out": noise(arg_keys[8], (D, D), D ** -0.5, 0.25, ((0, 16),)),
        "edge_gain": jnp.clip(1.0 + 0.18 * jax.random.normal(arg_keys[9], (D,), jnp.float32), 0.1, 1.9),
        "node_gain": jnp.clip(1.0 + 0.18 * jax.random.normal(arg_keys[10], (D,), jnp.float32), 0.1, 1.9),
        "node_cot": noise(arg_keys[11], (NODES, D), 1.0, 6.0, ((0, 256),)),
        "edge_cot": noise(arg_keys[12], (EDGES, D), 1.0, 6.0, ((0, 256),)),
    }


EPSILON = 1e-05

def apply_swish(values):
    return values * jax.nn.sigmoid(values)

def swish_slope(values):
    sigmoid_value = jax.nn.sigmoid(values)
    return sigmoid_value * (1.0 + values * (1.0 - sigmoid_value))

def layer_norm(values, gain_values):
    average = lax.optimization_barrier(jnp.mean(values, axis=1, keepdims=True))
    variance = lax.optimization_barrier(jnp.mean(values * values, axis=1, keepdims=True)) - average * average
    inverse = lax.rsqrt(variance + EPSILON)
    normed = (values - average) * inverse
    return (normed, inverse, normed * gain_values)

def layer_norm_back(cotangent, normed, inverse, gain_values):
    scaled = cotangent * gain_values
    first_mean = lax.optimization_barrier(jnp.mean(scaled, axis=1, keepdims=True))
    second_mean = lax.optimization_barrier(jnp.mean(scaled * normed, axis=1, keepdims=True))
    return (inverse * (scaled - first_mean - normed * second_mean)).astype(jnp.bfloat16)

def matmul(first_operand, second_operand):
    return jnp.dot(first_operand, second_operand, preferred_element_type=jnp.float32)

def matmul_back(first_operand, second_operand):
    return jnp.dot(first_operand, second_operand.T, preferred_element_type=jnp.float32)

def transposed(first_operand, second_operand):
    return jnp.dot(first_operand.T, second_operand, preferred_element_type=jnp.float32)

def reference(node_lat, edge_lat, receiver_row, sender_slot, send_rows, w_edge_in, w_edge_out, w_node_in, w_node_out, edge_gain, node_gain, node_cot, edge_cot):
    edge_region = (jnp.arange(EDGES, dtype=jnp.int32) // EDGE_DEV).astype(jnp.int32)
    receiver_index = (edge_region * NODE_DEV + receiver_row).astype(jnp.int32)
    remote = jnp.maximum(sender_slot - NODE_DEV, 0).astype(jnp.int32)
    peer_region = (remote // SLOTS).astype(jnp.int32)
    slot_index = (remote % SLOTS).astype(jnp.int32)
    remote_row = send_rows[peer_region, edge_region, slot_index]
    sender_index = jnp.where(sender_slot < NODE_DEV, edge_region * NODE_DEV + sender_slot, peer_region * NODE_DEV + remote_row).astype(jnp.int32)
    senders = node_lat[sender_index]
    receivers = node_lat[receiver_index]
    pre_hidden = matmul(edge_lat, w_edge_in[0]) + matmul(senders, w_edge_in[1]) + matmul(receivers, w_edge_in[2])
    hidden = apply_swish(pre_hidden).astype(jnp.bfloat16)
    edge_mix = matmul(hidden, w_edge_out)
    edge_normed, edge_inverse, edge_update = layer_norm(edge_mix, edge_gain)
    edge_new = (edge_lat.astype(jnp.float32) + edge_update).astype(jnp.bfloat16)
    pooled = jax.ops.segment_sum(edge_new.astype(jnp.float32), receiver_index, num_segments=NODES).astype(jnp.bfloat16)
    node_pre = matmul(node_lat, w_node_in[0]) + matmul(pooled, w_node_in[1])
    node_hidden = apply_swish(node_pre).astype(jnp.bfloat16)
    node_mix = matmul(node_hidden, w_node_out)
    node_normed, node_inverse, node_update = layer_norm(node_mix, node_gain)
    node_new = (node_lat.astype(jnp.float32) + node_update).astype(jnp.bfloat16)
    node_mix_grad = layer_norm_back(node_cot.astype(jnp.float32), node_normed, node_inverse, node_gain)
    node_pre_grad = (matmul_back(node_mix_grad, w_node_out) * swish_slope(node_pre)).astype(jnp.bfloat16)
    node_direct = matmul_back(node_pre_grad, w_node_in[0])
    pooled_grad = matmul_back(node_pre_grad, w_node_in[1])
    edge_total = edge_cot.astype(jnp.float32) + pooled_grad[receiver_index]
    edge_mix_grad = layer_norm_back(edge_total, edge_normed, edge_inverse, edge_gain)
    pre_grad = (matmul_back(edge_mix_grad, w_edge_out) * swish_slope(pre_hidden)).astype(jnp.bfloat16)
    edge_grad = edge_total + matmul_back(pre_grad, w_edge_in[0])
    sender_grad = matmul_back(pre_grad, w_edge_in[1])
    receiver_grad = matmul_back(pre_grad, w_edge_in[2])
    node_grad = node_cot.astype(jnp.float32) + node_direct + jax.ops.segment_sum(receiver_grad, receiver_index, num_segments=NODES) + jax.ops.segment_sum(sender_grad, sender_index, num_segments=NODES)
    edge_norm = 1.0 / jnp.sqrt(jnp.float32(EDGES))
    node_norm = 1.0 / jnp.sqrt(jnp.float32(NODES))
    grad_edge_in = jnp.stack([transposed(edge_lat, pre_grad), transposed(senders, pre_grad), transposed(receivers, pre_grad)], axis=0) * edge_norm
    grad_edge_out = transposed(hidden, edge_mix_grad) * edge_norm
    grad_node_in = jnp.stack([transposed(node_lat, node_pre_grad), transposed(pooled, node_pre_grad)], axis=0) * node_norm
    grad_node_out = transposed(node_hidden, node_mix_grad) * node_norm
    return (node_new, edge_new, node_grad, edge_grad, grad_edge_in, grad_edge_out, grad_node_in, grad_node_out)
```

```python
import jax
import jax.numpy as jnp
from jax import lax
from jax.experimental import pallas as pl
from jax.experimental.pallas import tpu as pltpu
from jax.sharding import PartitionSpec as P

MESH = pl.DeviceIdType.MESH
BF16, F32 = jnp.bfloat16, jnp.float32
EPSILON = 1e-05
SIDE = 4
EDGE_W, NODE_W = (0, 4), (4, 3)


def dot(a, b, da, db):
    return lax.dot_general(a, b, (((da,), (db,)), ((), ())), preferred_element_type=F32)


def mm(a, b):
    return dot(a, b, 1, 0)


def mm_back(a, b):
    return dot(a, b, 1, 1)


def mm_t(a, b):
    return dot(a, b, 0, 0)


def sigmoid(v):
    return 1.0 / (1.0 + jnp.exp(-v))


def layer_norm(m):
    width = m.shape[1]
    mean = jnp.sum(m, axis=1, keepdims=True) / width
    var = jnp.sum(m * m, axis=1, keepdims=True) / width - mean * mean
    inverse = lax.rsqrt(var + EPSILON)
    return (m - mean) * inverse, inverse


def layer_norm_back(cot, normed, inverse, gain):
    width = cot.shape[1]
    s = cot * gain
    first = jnp.sum(s, axis=1, keepdims=True) / width
    second = jnp.sum(s * normed, axis=1, keepdims=True) / width
    return (inverse * (s - first - normed * second)).astype(BF16)


def rows_equal(count, index, base=0):
    rows = lax.broadcasted_iota(jnp.int32, (count, index.shape[1]), 0) + base
    return jnp.where(rows == index, 1.0, 0.0).astype(BF16)


def kernel(regions, feats, scales,
           node, edge, recv_at, send_at, listed, wei, weo, wni, wno, egain, ngain, ncot, ecot,
           node_new, edge_new, node_grad, edge_grad, wgrad,
           nodes, gains, w, outgo, income, pre, normed, srows, rrows, hid, emg,
           pool_s, pool_r, npg, ng_s, ng_r, rem_s, rem_r, ret_s, ret_r, dist_s, dist_r,
           dw, pe_s, pe_r, pn_s, pn_r, re_s, re_r, rn_s, rn_r, qe_s, qe_r, qn_s, qn_r,
           ze_s, ze_r, zn_s, zn_r, be_s, be_r, bn_s, bn_r, ssem, rsem):
    g, f = lax.axis_index("region"), lax.axis_index("feat")
    c, z = lax.rem(g, 2), lax.div(g, 2)
    y, x = lax.div(f, SIDE), lax.rem(f, SIDE)
    sibling = g + 1 - 2 * c
    first = c == 0
    a = jnp.where(first, x, y)
    b = jnp.where(first, y, x)
    chips = regions // 2
    per = node.shape[0]
    width = node.shape[1]
    count = per * feats
    far = income.shape[0] * income.shape[1]

    def feat_at(a_, b_):
        return jnp.where(first, SIDE * b_ + a_, SIDE * a_ + b_)

    def send(src, dst, k, region, feat):
        return pltpu.make_async_remote_copy(
            src_ref=src, dst_ref=dst, send_sem=ssem.at[k], recv_sem=rsem.at[k],
            device_id=(region, feat), device_id_type=MESH)

    def to_plane(src_of, dst, k):
        def body(j, carry):
            t = lax.rem(f + j, feats)
            send(src_of(t), dst.at[f], k, g, t).start()
            return carry
        lax.fori_loop(1, feats, body, 0)

    def to_line(src_of, dst, k):
        def body(j, carry):
            t = lax.rem(g + j, regions)
            send(src_of(t), dst.at[g], k, t, f).start()
            return carry
        lax.fori_loop(1, regions, body, 0)

    def settle(view, k):
        send(view, view, k, g, f).wait()

    barrier = pltpu.get_barrier_semaphore()

    def greet(j, carry):
        pl.semaphore_signal(barrier, inc=1, device_id=(g, lax.rem(f + j, feats)), device_id_type=MESH)
        pl.semaphore_signal(barrier, inc=1, device_id=(lax.rem(g + j, regions), f), device_id_type=MESH)
        return carry
    lax.fori_loop(1, feats, greet, 0)

    lanes = lax.broadcasted_iota(jnp.int32, (egain.shape[1], width), 1)
    lines = lax.broadcasted_iota(jnp.int32, (egain.shape[1], width), 0)
    place = jnp.where(lanes == lines + f * egain.shape[1], 1.0, 0.0)
    both = jnp.concatenate([egain[...], ngain[...]], axis=0)
    gains[f] = lax.dot_general(both, place, (((1,), (0,)), ((), ())), precision=lax.Precision.HIGHEST,
                               preferred_element_type=F32)
    nodes[f] = node[...]
    for k in range(3):
        w[k, y, x, c] = wei[k, c]
    w[3, y, x, c] = weo[c]
    for k in range(2):
        w[4 + k, y, x, c] = wni[k, c]
    w[6, y, x, c] = wno[c]
    income[g] = jnp.zeros(income.shape[1:], BF16)
    ret_r[g] = jnp.zeros(ret_r.shape[1:], BF16)
    pl.semaphore_wait(barrier, feats - 1 + regions - 1)

    to_plane(lambda t: node, nodes, 0)
    to_plane(lambda t: gains.at[f], gains, 1)

    def weights_first(group, k):
        ks = pl.ds(*group)
        for d in range(1, SIDE):
            t = feat_at(lax.rem(a + d, SIDE), b)
            send(w.at[ks, y, x, c], w.at[ks, y, x, c], k, g, t).start()

    def weights_second(group, k, k2):
        ks = pl.ds(*group)
        settle(w.at[ks, 0, pl.ds(0, SIDE - 1), 0], k)

        @pl.when(first)
        def _():
            for d in range(1, SIDE):
                part = w.at[ks, y, :, 0]
                send(part, part, k2, g, SIDE * lax.rem(y + d, SIDE) + x).start()

        @pl.when(c == 1)
        def _():
            for d in range(1, SIDE):
                part = w.at[ks, :, x, 1]
                send(part, part, k2, g, SIDE * y + lax.rem(x + d, SIDE)).start()

    def weights_pass(group, k2, k3):
        ks = pl.ds(*group)
        settle(w.at[ks, pl.ds(0, SIDE - 1), :, 0], k2)
        send(w.at[ks, :, :, c], w.at[ks, :, :, c], k3, sibling, f).start()

    def weights_end(group, k3):
        settle(w.at[pl.ds(*group), :, :, 0], k3)

    weights_first(EDGE_W, 2)
    settle(nodes.at[pl.ds(0, feats - 1)], 0)
    table = nodes[...].reshape(count, width)
    picked = mm_t(rows_equal(count, listed[...]), table).astype(BF16)
    outgo[...] = picked.reshape(outgo.shape)
    to_line(lambda t: outgo.at[t], income, 3)
    weights_second(EDGE_W, 2, 4)
    weights_first(NODE_W, 5)

    into = rows_equal(count, recv_at[...])
    near = rows_equal(count, send_at[...])
    rrows[...] = mm_t(into, table).astype(BF16)
    near_rows = mm_t(near, table)

    weights_pass(EDGE_W, 4, 6)
    weights_second(NODE_W, 5, 7)
    settle(income.at[pl.ds(0, regions - 1)], 3)
    away = rows_equal(far, send_at[...], count)
    srows[...] = (near_rows + mm_t(away, income[...].reshape(far, width))).astype(BF16)
    settle(gains.at[pl.ds(0, feats - 1)], 1)
    gain = jnp.sum(gains[...], axis=0)
    weights_end(EDGE_W, 6)

    def weight(k):
        return w[k].reshape(width, width)

    pre[...] = mm(edge[...], weight(0)) + mm(srows[...], weight(1)) + mm(rrows[...], weight(2))
    hid[...] = (pre[...] * sigmoid(pre[...])).astype(BF16)
    edge_normed, edge_inverse = layer_norm(mm(hid[...], weight(3)))
    normed[...] = edge_normed
    fresh = (edge[...].astype(F32) + edge_normed * gain[0:1]).astype(BF16)
    edge_new[...] = fresh
    pool_s[...] = mm(into, fresh).astype(BF16).reshape(pool_s.shape)
    pool_r[f] = pool_s[f]
    to_plane(lambda t: pool_s.at[t], pool_r, 8)
    weights_pass(NODE_W, 7, 9)
    weights_end(NODE_W, 9)
    settle(pool_r.at[pl.ds(0, feats - 1)], 8)

    pooled = jnp.sum(pool_r[...].astype(F32), axis=0).astype(BF16)
    lat = node[...]
    node_pre = mm(lat, weight(4)) + mm(pooled, weight(5))
    gate = sigmoid(node_pre)
    node_hid = (node_pre * gate).astype(BF16)
    node_normed, node_inverse = layer_norm(mm(node_hid, weight(6)))
    node_new[...] = (lat.astype(F32) + node_normed * gain[1:2]).astype(BF16)
    nmg = layer_norm_back(ncot[...].astype(F32), node_normed, node_inverse, gain[1:2])
    slope = gate * (1.0 + node_pre * (1.0 - gate))
    own_npg = (mm_back(nmg, weight(6)) * slope).astype(BF16)
    npg[f] = own_npg
    to_plane(lambda t: npg.at[f], npg, 10)

    def trade(group, products, out, back, k):
        start, n = group
        for i in range(n):
            dw[start + i] = products(i).reshape(dw.shape[1:])
            out[i] = dw[start + i, :, 1 - c].astype(BF16)
        send(out, back, k, sibling, f).start()

    def along_a(group, out, back, stage, landed, k, k2):
        start, n = group
        settle(back, k)

        def body(j, carry):
            a_, b_ = lax.div(j, SIDE), lax.rem(j, SIDE)
            at = feat_at(a_, b_)
            for i in range(n):
                stage[a_, i, b_] = (dw[start + i, at, c] + back[i, at].astype(F32)).astype(BF16)
            return carry
        lax.fori_loop(0, feats, body, 0)
        landed[a] = stage[a]
        for d in range(1, SIDE):
            a_ = lax.rem(a + d, SIDE)
            send(stage.at[a_], landed.at[a], k2, g, feat_at(a_, b)).start()

    def along_b(landed, stage, landed2, k2, k3):
        settle(landed.at[pl.ds(0, SIDE - 1)], k2)

        def body(b_, carry):
            stage[b_] = jnp.sum(landed[:, :, b_].astype(F32), axis=0).astype(BF16)
            return carry
        lax.fori_loop(0, SIDE, body, 0)
        landed2[b] = stage[b]
        for d in range(1, SIDE):
            b_ = lax.rem(b + d, SIDE)
            send(stage.at[b_], landed2.at[b], k3, g, feat_at(a, b_)).start()

    def along_z(landed, stage, landed2, k3, k4):
        settle(landed.at[pl.ds(0, SIDE - 1)], k3)
        stage[...] = jnp.sum(landed[...].astype(F32), axis=0).astype(BF16)
        landed2[z] = stage[...]
        for d in range(1, chips):
            send(stage, landed2.at[z], k4, lax.rem(g + 2 * d, regions), f).start()

    def to_sibling(group, landed, stage, landed2, k4, k5, scale):
        settle(landed.at[pl.ds(0, chips - 1)], k4)
        stage[...] = jnp.sum(landed[...].astype(F32), axis=0) * scale
        send(stage, landed2, k5, sibling, f).start()
        wgrad[pl.ds(*group), c] = stage[...]

    def finish(group, landed, k5):
        settle(landed, k5)
        wgrad[pl.ds(*group), 1 - c] = landed[...]

    node_sides = ((lat, own_npg), (pooled, own_npg), (node_hid, nmg))
    trade(NODE_W, lambda i: mm_t(*node_sides[i]), pn_s, pn_r, 11)
    direct = ncot[...].astype(F32) + mm_back(own_npg, weight(4))
    along_a(NODE_W, pn_s, pn_r, rn_s, rn_r, 11, 12)
    settle(npg.at[pl.ds(0, feats - 1)], 10)

    reached = mm_t(into, npg[...].reshape(count, width)).astype(BF16)
    total = ecot[...].astype(F32) + mm_back(reached, weight(5))
    emg[...] = layer_norm_back(total, normed[...], edge_inverse, gain[0:1])
    gate = sigmoid(pre[...])
    slope = gate * (1.0 + pre[...] * (1.0 - gate))
    pre_grad = (mm_back(emg[...], weight(3)) * slope).astype(BF16)
    from_send = mm_back(pre_grad, weight(1)).astype(BF16)
    from_recv = mm_back(pre_grad, weight(2)).astype(BF16)
    rem_s[...] = mm(away, from_send).astype(BF16).reshape(rem_s.shape)
    rem_r[f] = rem_s[f]
    to_plane(lambda t: rem_s.at[t], rem_r, 13)
    ng_s[...] = (mm(near, from_send) + mm(into, from_recv)).astype(BF16).reshape(ng_s.shape)
    ng_r[f] = ng_s[f]
    to_plane(lambda t: ng_s.at[t], ng_r, 14)
    edge_grad[...] = total + mm_back(pre_grad, weight(0))
    edge_sides = ((edge, None), (srows, None), (rrows, None), (hid, emg))
    trade(EDGE_W, lambda i: mm_t(edge_sides[i][0][...], pre_grad if i < 3 else emg[...]), pe_s, pe_r, 15)
    along_b(rn_r, qn_s, qn_r, 12, 16)
    along_a(EDGE_W, pe_s, pe_r, re_s, re_r, 15, 17)

    settle(rem_r.at[pl.ds(0, feats - 1)], 13)
    ret_s[...] = jnp.sum(rem_r[...].astype(F32), axis=0).astype(BF16)

    @pl.when(g != f)
    def _():
        send(ret_s, ret_r.at[g], 18, f, f).start()

    along_z(qn_r, zn_s, zn_r, 16, 19)
    along_b(re_r, qe_s, qe_r, 17, 20)

    @pl.when(g == f)
    def _():
        send(ret_r.at[pl.ds(0, regions - 1)], ret_r.at[pl.ds(0, regions - 1)], 18, g, f).wait_recv()
        back = mm(rows_equal(count, listed[...]), ret_r[...].reshape(far, width))
        dist_s[...] = back.astype(BF16).reshape(dist_s.shape)
        dist_r[...] = dist_s[f]
        for d in range(1, feats):
            t = lax.rem(f + d, feats)
            send(dist_s.at[t], dist_r, 21, g, t).start()

    along_z(qe_r, ze_s, ze_r, 20, 22)
    settle(ng_r.at[pl.ds(0, feats - 1)], 14)

    @pl.when(g != f)
    def _():
        send(ret_s, ret_s, 18, f, f).wait_send()
        send(dist_r, dist_r, 21, g, f).wait_recv()

    node_grad[...] = direct + jnp.sum(ng_r[...].astype(F32), axis=0) + dist_r[...].astype(F32)
    to_sibling(NODE_W, zn_r, bn_s, bn_r, 19, 23, scales[1])
    to_sibling(EDGE_W, ze_r, be_s, be_r, 22, 24, scales[0])
    finish(NODE_W, bn_r, 23)
    finish(EDGE_W, be_r, 24)

    @pl.when(g == f)
    def _():
        send(dist_s.at[pl.ds(0, feats - 1)], dist_s.at[pl.ds(0, feats - 1)], 21, g, f).wait_send()


def shards(sizes, node_lat, edge_lat, receiver_row, sender_slot, send_rows, w_edge_in, w_edge_out, w_node_in,
           w_node_out, edge_gain, node_gain, node_cot, edge_cot):
    regions, feats = sizes
    per, width = node_lat.shape
    edges = edge_lat.shape[0]
    slots = send_rows.shape[2]
    part = width // feats // 2
    f = lax.axis_index("feat")
    recv_at = lax.dynamic_slice_in_dim(receiver_row, f * edges, edges)[None]
    send_at = lax.dynamic_slice_in_dim(sender_slot, f * edges, edges)[None]
    listed = send_rows.reshape(1, regions * slots)
    scales = (1.0 / float(edges * feats * regions) ** 0.5, 1.0 / float(per * feats * regions) ** 0.5)
    ne, nn = EDGE_W[1], NODE_W[1]

    def v(dtype, *shape):
        return pltpu.VMEM(shape, dtype)

    nodes_like = (feats, per, width)
    line_like = (regions, slots, width)

    def pair(dtype, *shape):
        return [v(dtype, *shape)] * 2

    scratch = [
        v(BF16, *nodes_like), v(F32, feats, 2, width), v(BF16, ne + nn, SIDE, SIDE, 2, part, width),
        *pair(BF16, *line_like),
        *pair(F32, edges, width),
        *[v(BF16, edges, width)] * 4,
        *pair(BF16, *nodes_like), v(BF16, *nodes_like), *pair(BF16, *nodes_like), *pair(BF16, *line_like),
        v(BF16, slots, width), v(BF16, *line_like), v(BF16, *nodes_like), v(BF16, per, width),
        v(F32, ne + nn, feats, 2, part, width),
        *pair(BF16, ne, feats, part, width), *pair(BF16, nn, feats, part, width),
        *pair(BF16, SIDE, ne, SIDE, part, width), *pair(BF16, SIDE, nn, SIDE, part, width),
        *pair(BF16, SIDE, ne, part, width), *pair(BF16, SIDE, nn, part, width),
        v(BF16, ne, part, width), v(BF16, regions // 2, ne, part, width),
        v(BF16, nn, part, width), v(BF16, regions // 2, nn, part, width),
        *pair(F32, ne, part, width), *pair(F32, nn, part, width),
        pltpu.SemaphoreType.DMA((25,)), pltpu.SemaphoreType.DMA((25,)),
    ]

    def body(*refs):
        kernel(regions, feats, scales, *refs)

    vmem = pl.BlockSpec(memory_space=pltpu.VMEM)
    node_new, edge_new, node_grad, edge_grad, wgrad = pl.pallas_call(
        body,
        name="layer",
        out_shape=(
            jax.ShapeDtypeStruct((per, width), BF16), jax.ShapeDtypeStruct((edges, width), BF16),
            jax.ShapeDtypeStruct((per, width), F32), jax.ShapeDtypeStruct((edges, width), F32),
            jax.ShapeDtypeStruct((ne + nn, 2, part, width), F32),
        ),
        in_specs=[vmem] * 13,
        out_specs=[vmem] * 5,
        scratch_shapes=scratch,
        compiler_params=pltpu.CompilerParams(
            collective_id=0, has_side_effects=True, vmem_limit_bytes=60 * 2**20),
    )(node_lat, edge_lat, recv_at, send_at, listed,
      w_edge_in.reshape(3, 2, part, width), w_edge_out.reshape(2, part, width),
      w_node_in.reshape(2, 2, part, width), w_node_out.reshape(2, part, width),
      edge_gain[None], node_gain[None], node_cot, edge_cot)
    wgrad = wgrad.reshape(ne + nn, 2 * part, width)
    return node_new, edge_new, node_grad, edge_grad, wgrad[:3], wgrad[3], wgrad[4:6], wgrad[6]


def solution(mesh):
    rows = P(("region", "feat"), None)
    blocks = (P(None, "feat", None), P("feat", None), P(None, "feat", None), P("feat", None))
    in_specs = (rows, rows, P("region"), P("region"), P("region", None, None), *blocks, P("feat"), P("feat"), rows, rows)
    sizes = (mesh.shape["region"], mesh.shape["feat"])
    return jax.shard_map(lambda *args: shards(sizes, *args), mesh=mesh, in_specs=in_specs,
                         out_specs=(rows, rows, rows, rows, *blocks), check_vma=False)
```

```python
import jax
import jax.numpy as jnp
from jax import lax
from jax.experimental import pallas as pl
from jax.experimental.pallas import tpu as pltpu
from jax.sharding import PartitionSpec as P

MESH = pl.DeviceIdType.MESH
BF16, F32 = jnp.bfloat16, jnp.float32
EPSILON = 1e-05
SIDE = 4
EDGE_W, NODE_W = (0, 4), (4, 3)
VMEM_LIMIT = 44 * 2**20


def dot(a, b, da, db):
    return lax.dot_general(a, b, (((da,), (db,)), ((), ())), preferred_element_type=F32)


def mm(a, b):
    return dot(a, b, 1, 0)


def mm_back(a, b):
    return dot(a, b, 1, 1)


def mm_t(a, b):
    return dot(a, b, 0, 0)


def sigmoid(v):
    return 1.0 / (1.0 + jnp.exp(-v))


def layer_norm(m):
    width = m.shape[1]
    mean = jnp.sum(m, axis=1, keepdims=True) / width
    var = jnp.sum(m * m, axis=1, keepdims=True) / width - mean * mean
    inverse = lax.rsqrt(var + EPSILON)
    return (m - mean) * inverse, inverse


def layer_norm_back(cot, normed, inverse, gain):
    width = cot.shape[1]
    s = cot * gain
    first = jnp.sum(s, axis=1, keepdims=True) / width
    second = jnp.sum(s * normed, axis=1, keepdims=True) / width
    return (inverse * (s - first - normed * second)).astype(BF16)


def iota(shape, dim):
    return lax.broadcasted_iota(jnp.int32, shape, dim)


def rows_equal(count, index, base=0):
    rows = iota((count, index.shape[1]), 0) + base
    return jnp.where(rows == index, 1.0, 0.0).astype(BF16)


def flat(blocks, pick, mine):
    wide = lax.dot_general(blocks, jnp.where(pick, 1.0, 0.0), (((1,), (0,)), ((), ())),
                           precision=lax.Precision.HIGHEST, preferred_element_type=F32)
    return jnp.sum(jnp.where(mine, wide, 0.0), axis=0, keepdims=True)


def own_slice(ref, f, edges):
    lines = 2 * edges // 128
    start = lax.div(f, 2) * lines
    two = jnp.concatenate([ref[start + i] for i in range(lines)], axis=1)
    return jnp.where(lax.rem(f, 2) == 1, two[:, edges:], two[:, :edges])


def kernel(regions, feats, scales, fetches,
           node, edge, recv_all, send_all, listed_at, wei, weo, wni, wno, egain, ngain, ncot, ecot,
           node_new, edge_new, node_grad, edge_grad, wgrad,
           nodes, gains, w, outgo, income, pre, normed, srows, rrows, hid, emg,
           pool_s, pool_r, npg, ng_s, ng_r, rem_s, rem_r, ret_s, ret_r, dist_s, dist_r,
           dw, pe_s, pe_r, pn_s, pn_r, re_s, re_r, rn_s, rn_r, qe_s, qe_r, qn_s, qn_r,
           ze_s, ze_r, zn_s, zn_r, be, bn, ssem, rsem):
    g, f = lax.axis_index("region"), lax.axis_index("feat")
    c, z = lax.rem(g, 2), lax.div(g, 2)
    y, x = lax.div(f, SIDE), lax.rem(f, SIDE)
    sibling = g + 1 - 2 * c
    first = c == 0
    a = jnp.where(first, x, y)
    b = jnp.where(first, y, x)
    chips = regions // 2
    per, width = node.shape
    edges = edge.shape[0]
    count = per * feats
    slots = income.shape[1]
    far = regions * slots

    def feat_at(a_, b_):
        return jnp.where(first, SIDE * b_ + a_, SIDE * a_ + b_)

    def send(src, dst, k, region, feat):
        return pltpu.make_async_remote_copy(
            src_ref=src, dst_ref=dst, send_sem=ssem.at[k], recv_sem=rsem.at[k],
            device_id=(region, feat), device_id_type=MESH)

    def to_plane(src_of, dst, k):
        def body(j, carry):
            t = lax.rem(f + j, feats)
            send(src_of(t), dst.at[f], k, g, t).start()
            return carry
        lax.fori_loop(1, feats, body, 0)

    def to_line(src_of, dst, k):
        def body(j, carry):
            t = lax.rem(g + j, regions)
            send(src_of(t), dst.at[g], k, t, f).start()
            return carry
        lax.fori_loop(1, regions, body, 0)

    def settle(view, k):
        send(view, view, k, g, f).wait()

    def settle_slots(buffer, k):
        settle(buffer.at[pl.ds(0, buffer.shape[0] - 1)], k)

    barrier = pltpu.get_barrier_semaphore()

    def greet(j, carry):
        pl.semaphore_signal(barrier, inc=1, device_id=(g, lax.rem(f + j, feats)), device_id_type=MESH)
        pl.semaphore_signal(barrier, inc=1, device_id=(lax.rem(g + j, regions), f), device_id_type=MESH)
        return carry
    lax.fori_loop(1, feats, greet, 0)
    for fetch in fetches:
        fetch.wait()

    portion = egain.shape[1]
    gains[f] = jnp.concatenate([egain[...], ngain[...], jnp.zeros((1, gains.shape[2] - 2 * portion), F32)], axis=1)
    nodes[f] = node[...]
    for k in range(3):
        w[k, y, x, c] = wei[k, c]
    w[3, y, x, c] = weo[c]
    for k in range(2):
        w[4 + k, y, x, c] = wni[k, c]
    w[6, y, x, c] = wno[c]
    income[g] = jnp.zeros(income.shape[1:], BF16)
    ret_r[g] = jnp.zeros(ret_r.shape[1:], BF16)
    recv_at = own_slice(recv_all, f, edges)
    send_at = own_slice(send_all, f, edges)
    grid = (regions, far)
    listed = flat(listed_at[0].astype(F32), lax.rem(iota((slots, far), 1), slots) == iota((slots, far), 0),
                  lax.div(iota(grid, 1), slots) == iota(grid, 0))
    asked = jnp.where(iota((count, far), 0).astype(F32) == listed, 1.0, 0.0).astype(BF16)
    into = rows_equal(count, recv_at)
    near = rows_equal(count, send_at)
    away = rows_equal(far, send_at, count)
    pl.semaphore_wait(barrier, feats - 1 + regions - 1)

    def weights_first(group, k):
        part = w.at[pl.ds(*group), y, x, c]
        for d in range(1, SIDE):
            send(part, part, k, g, feat_at(lax.rem(a + d, SIDE), b)).start()

    def bundle(group, b_, act):
        ks = pl.ds(*group)

        @pl.when(first)
        def _():
            act(w.at[ks, b_, :, 0])

        @pl.when(c == 1)
        def _():
            act(w.at[ks, :, b_, 1])

    def weights_second(group, k, k2):
        settle(w.at[pl.ds(*group), 0, pl.ds(0, SIDE - 1), 0], k)

        def act(part):
            for d in range(1, SIDE):
                send(part, part, k2 + d, g, feat_at(a, lax.rem(b + d, SIDE))).start()
            send(part, part, k2, sibling, f).start()
        bundle(group, b, act)

    def weights_pass(group, k2):
        for d in range(1, SIDE):
            settle(w.at[pl.ds(*group), 0, :, 0], k2 + d)
            bundle(group, lax.rem(b - d + SIDE, SIDE), lambda part: send(part, part, k2, sibling, f).start())

    def weights_end(group, k2):
        settle(w.at[pl.ds(*group), :, :, 0], k2)

    to_plane(lambda t: node, nodes, 0)
    weights_first(EDGE_W, 2)
    weights_first(NODE_W, 3)
    to_plane(lambda t: gains.at[f], gains, 1)
    settle_slots(nodes, 0)
    table = nodes[...].reshape(count, width)
    outgo[...] = mm_t(asked, table).astype(BF16).reshape(outgo.shape)
    to_line(lambda t: outgo.at[t], income, 4)
    weights_second(EDGE_W, 2, 5)
    weights_second(NODE_W, 3, 9)
    rrows[...] = mm_t(into, table).astype(BF16)
    near_rows = mm_t(near, table)
    settle_slots(gains, 1)
    packed = gains[...].reshape(feats, gains.shape[2])
    shape, wide = (gains.shape[2], 2 * width), (feats, 2 * width)
    lanes = iota(shape, 1)
    gain = flat(packed, lax.rem(lanes, portion) + portion * lax.div(lanes, width) == iota(shape, 0),
                lax.div(lax.rem(iota(wide, 1), width), portion) == iota(wide, 0))
    edge_gain, node_gain = gain[:, :width], gain[:, width:]
    weights_pass(EDGE_W, 5)
    settle_slots(income, 4)
    srows[...] = (near_rows + mm_t(away, income[...].reshape(far, width))).astype(BF16)
    weights_end(EDGE_W, 5)

    def weight(k):
        return w[k].reshape(width, width)

    pre[...] = mm(edge[...], weight(0)) + mm(srows[...], weight(1)) + mm(rrows[...], weight(2))
    hid[...] = (pre[...] * sigmoid(pre[...])).astype(BF16)
    edge_normed, edge_inverse = layer_norm(mm(hid[...], weight(3)))
    normed[...] = edge_normed
    fresh = (edge[...].astype(F32) + edge_normed * edge_gain).astype(BF16)
    edge_new[...] = fresh
    pool_s[...] = mm(into, fresh).astype(BF16).reshape(pool_s.shape)
    pool_r[f] = pool_s[f]
    to_plane(lambda t: pool_s.at[t], pool_r, 13)
    weights_pass(NODE_W, 9)
    weights_end(NODE_W, 9)
    settle_slots(pool_r, 13)

    pooled = jnp.sum(pool_r[...].astype(F32), axis=0).astype(BF16)
    lat = node[...]
    node_pre = mm(lat, weight(4)) + mm(pooled, weight(5))
    gate = sigmoid(node_pre)
    node_hid = (node_pre * gate).astype(BF16)
    node_normed, node_inverse = layer_norm(mm(node_hid, weight(6)))
    node_new[...] = (lat.astype(F32) + node_normed * node_gain).astype(BF16)
    nmg = layer_norm_back(ncot[...].astype(F32), node_normed, node_inverse, node_gain)
    slope = gate * (1.0 + node_pre * (1.0 - gate))
    own_npg = (mm_back(nmg, weight(6)) * slope).astype(BF16)
    npg[f] = own_npg
    to_plane(lambda t: npg.at[f], npg, 14)

    def trade(group, products, out, back, k):
        start, n = group
        for i in range(n):
            dw[start + i] = products(i).reshape(dw.shape[1:])
            out[i] = dw[start + i, :, 1 - c].astype(BF16)
        send(out, back, k, sibling, f).start()

    def along_a(group, out, back, stage, landed, k, k2):
        start, n = group
        settle(back, k)

        def body(j, carry):
            a_, b_ = lax.div(j, SIDE), lax.rem(j, SIDE)
            at = feat_at(a_, b_)
            for i in range(n):
                stage[a_, i, b_] = (dw[start + i, at, c] + back[i, at].astype(F32)).astype(BF16)
            return carry
        lax.fori_loop(0, feats, body, 0)
        landed[a] = stage[a]
        for d in range(1, SIDE):
            a_ = lax.rem(a + d, SIDE)
            send(stage.at[a_], landed.at[a], k2, g, feat_at(a_, b)).start()

    def along_b(landed, stage, landed2, k2, k3):
        settle_slots(landed, k2)

        def body(b_, carry):
            stage[b_] = jnp.sum(landed[:, :, b_].astype(F32), axis=0).astype(BF16)
            return carry
        lax.fori_loop(0, SIDE, body, 0)
        landed2[b] = stage[b]
        for d in range(1, SIDE):
            b_ = lax.rem(b + d, SIDE)
            send(stage.at[b_], landed2.at[b], k3, g, feat_at(a, b_)).start()

    def along_z(landed, stage, landed2, k3, k4):
        settle_slots(landed, k3)
        whole = jnp.sum(landed[...].astype(F32), axis=0).astype(BF16)
        rows = stage.shape[1]
        pieces = whole.reshape(whole.shape[0] * whole.shape[1] // rows, rows, width)
        stage[pl.ds(0, pieces.shape[0])] = pieces
        if pieces.shape[0] < chips:
            stage[pl.ds(pieces.shape[0], chips - pieces.shape[0])] = jnp.zeros(
                (chips - pieces.shape[0], rows, width), BF16)
        landed2[z] = stage[z]
        for d in range(1, chips):
            z_ = lax.rem(z + d, chips)
            send(stage.at[z_], landed2.at[z], k4, 2 * z_ + c, f).start()

    def to_all(landed, whole, k4, k5, scale):
        settle_slots(landed, k4)
        whole[g] = (jnp.sum(landed[...].astype(F32), axis=0) * scale).astype(BF16)
        to_line(lambda t: whole.at[g], whole, k5)

    def finish(group, whole, k5):
        settle_slots(whole, k5)
        start, n = group
        rows = whole.shape[1]
        halves = wgrad.shape[2] // rows
        for i in range(n):
            for c_ in range(2):
                for h in range(halves):
                    wgrad[start + i, c_, pl.ds(h * rows, rows)] = whole[2 * (halves * i + h) + c_].astype(F32)

    node_sides = ((lat, own_npg), (pooled, own_npg), (node_hid, nmg))
    trade(NODE_W, lambda i: mm_t(*node_sides[i]), pn_s, pn_r, 15)
    direct = ncot[...].astype(F32) + mm_back(own_npg, weight(4))
    along_a(NODE_W, pn_s, pn_r, rn_s, rn_r, 15, 16)
    settle_slots(npg, 14)

    reached = mm_t(into, npg[...].reshape(count, width)).astype(BF16)
    total = ecot[...].astype(F32) + mm_back(reached, weight(5))
    emg[...] = layer_norm_back(total, normed[...], edge_inverse, edge_gain)
    gate = sigmoid(pre[...])
    slope = gate * (1.0 + pre[...] * (1.0 - gate))
    pre_grad = (mm_back(emg[...], weight(3)) * slope).astype(BF16)
    edge_sides = ((edge, None), (srows, None), (rrows, None), (hid, emg))
    trade(EDGE_W, lambda i: mm_t(edge_sides[i][0][...], pre_grad if i < 3 else emg[...]), pe_s, pe_r, 17)
    from_send = mm_back(pre_grad, weight(1)).astype(BF16)
    rem_s[...] = mm(away, from_send).astype(BF16).reshape(rem_s.shape)
    rem_r[f] = rem_s[f]
    to_plane(lambda t: rem_s.at[t], rem_r, 18)
    from_recv = mm_back(pre_grad, weight(2)).astype(BF16)
    ng_s[...] = (mm(near, from_send) + mm(into, from_recv)).astype(BF16).reshape(ng_s.shape)
    ng_r[f] = ng_s[f]
    edge_grad[...] = total + mm_back(pre_grad, weight(0))
    along_a(EDGE_W, pe_s, pe_r, re_s, re_r, 17, 19)
    along_b(rn_r, qn_s, qn_r, 16, 20)
    to_plane(lambda t: ng_s.at[t], ng_r, 21)

    settle_slots(rem_r, 18)
    ret_s[...] = jnp.sum(rem_r[...].astype(F32), axis=0).astype(BF16)

    @pl.when(g != f)
    def _():
        send(ret_s, ret_r.at[g], 22, f, f).start()

    along_z(qn_r, zn_s, zn_r, 20, 23)
    along_b(re_r, qe_s, qe_r, 19, 24)

    @pl.when(g == f)
    def _():
        send(ret_r.at[pl.ds(0, regions - 1)], ret_r.at[pl.ds(0, regions - 1)], 22, g, f).wait_recv()
        dist_s[...] = mm(asked, ret_r[...].reshape(far, width)).astype(BF16).reshape(dist_s.shape)
        dist_r[...] = dist_s[f]
        for d in range(1, feats):
            t = lax.rem(f + d, feats)
            send(dist_s.at[t], dist_r, 25, g, t).start()

    along_z(qe_r, ze_s, ze_r, 24, 26)
    to_all(zn_r, bn, 23, 27, scales[1])
    to_all(ze_r, be, 26, 28, scales[0])
    settle_slots(ng_r, 21)

    @pl.when(g != f)
    def _():
        send(ret_s, ret_s, 22, f, f).wait_send()
        send(dist_r, dist_r, 25, g, f).wait_recv()

    node_grad[...] = direct + jnp.sum(ng_r[...].astype(F32), axis=0) + dist_r[...].astype(F32)
    finish(NODE_W, bn, 27)
    finish(EDGE_W, be, 28)

    @pl.when(g == f)
    def _():
        send(dist_s.at[pl.ds(0, feats - 1)], dist_s.at[pl.ds(0, feats - 1)], 25, g, f).wait_send()


def hand_on(*refs):
    sources, outs, out = refs[:5], refs[5:13], refs[13]
    grads = sources[4]
    views = [*sources[:4], grads.at[pl.ds(0, 3)], grads.at[3], grads.at[pl.ds(4, 2)], grads.at[6]]
    copies = [pltpu.make_async_copy(v, o, out.at[i]) for i, (v, o) in enumerate(zip(views, outs))]
    for copy in copies:
        copy.start()
    for copy in copies:
        copy.wait()


def shards(sizes, node_lat, edge_lat, receiver_row, sender_slot, send_rows, w_edge_in, w_edge_out, w_node_in,
           w_node_out, edge_gain, node_gain, node_cot, edge_cot):
    regions, feats = sizes
    per, width = node_lat.shape
    edges = edge_lat.shape[0]
    slots = send_rows.shape[2]
    part = width // feats // 2
    lines = (edges * feats // 128, 1, 128)
    scales = (1.0 / float(edges * feats * regions) ** 0.5, 1.0 / float(per * feats * regions) ** 0.5)
    ne, nn = EDGE_W[1], NODE_W[1]
    piece = ne * part // (regions // 2)

    def v(dtype, *shape):
        return pltpu.VMEM(shape, dtype)

    nodes_like = (feats, per, width)
    line_like = (regions, slots, width)

    def pair(dtype, *shape):
        return [v(dtype, *shape)] * 2

    scratch = [
        v(BF16, *nodes_like), v(F32, feats, 1, 128), v(BF16, ne + nn, SIDE, SIDE, 2, part, width),
        *pair(BF16, *line_like),
        *pair(F32, edges, width),
        *[v(BF16, edges, width)] * 4,
        *pair(BF16, *nodes_like), v(BF16, *nodes_like), *pair(BF16, *nodes_like), *pair(BF16, *line_like),
        v(BF16, slots, width), v(BF16, *line_like), v(BF16, *nodes_like), v(BF16, per, width),
        v(F32, ne + nn, feats, 2, part, width),
        *pair(BF16, ne, feats, part, width), *pair(BF16, nn, feats, part, width),
        *pair(BF16, SIDE, ne, SIDE, part, width), *pair(BF16, SIDE, nn, SIDE, part, width),
        *pair(BF16, SIDE, ne, part, width), *pair(BF16, SIDE, nn, part, width),
        *pair(BF16, regions // 2, piece, width), *pair(BF16, regions // 2, piece, width),
        *pair(BF16, regions, piece, width),
        pltpu.SemaphoreType.DMA((29,)), pltpu.SemaphoreType.DMA((29,)),
    ]

    args = (node_lat, edge_lat, receiver_row.reshape(lines), sender_slot.reshape(lines), send_rows,
            w_edge_in.reshape(3, 2, part, width), w_edge_out.reshape(2, part, width),
            w_node_in.reshape(2, 2, part, width), w_node_out.reshape(2, part, width),
            edge_gain[None], node_gain[None], node_cot, edge_cot)
    n = len(args)
    scratch += [*[v(x.dtype, *x.shape) for x in args], pltpu.SemaphoreType.DMA((n,))]

    def body(*refs):
        sources, rest = refs[:n], refs[n:]
        held, sem = rest[-n - 1:-1], rest[-1]
        fetches = [pltpu.make_async_copy(s, h, sem.at[i]) for i, (s, h) in enumerate(zip(sources, held))]
        for fetch in fetches:
            fetch.start()
        kernel(regions, feats, scales, fetches, *held, *rest[:-n - 1])

    vmem = pl.BlockSpec(memory_space=pltpu.VMEM)
    kinds = [((per, width), BF16), ((edges, width), BF16), ((per, width), F32), ((edges, width), F32)]
    blocks = [(3, 2, part, width), (2, part, width), (2, 2, part, width), (2, part, width)]
    results = pl.pallas_call(
        body,
        name="layer",
        out_shape=[jax.ShapeDtypeStruct(*k) for k in (*kinds, ((ne + nn, 2, part, width), F32))],
        in_specs=[pl.BlockSpec(memory_space=pltpu.HBM)] * n,
        out_specs=[vmem] * 5,
        scratch_shapes=scratch,
        compiler_params=pltpu.CompilerParams(
            collective_id=0, has_side_effects=True, vmem_limit_bytes=VMEM_LIMIT),
    )(*[pltpu.with_memory_space_constraint(x, pltpu.HBM) for x in args])
    kinds += [(s, F32) for s in blocks]
    outs = pl.pallas_call(
        hand_on,
        name="hand_on",
        out_shape=[jax.ShapeDtypeStruct(*k) for k in kinds],
        in_specs=[vmem] * 5,
        out_specs=[pl.BlockSpec(memory_space=pltpu.HBM)] * 8,
        scratch_shapes=[pltpu.SemaphoreType.DMA((8,))],
        compiler_params=pltpu.CompilerParams(vmem_limit_bytes=8 * 2**20),
    )(*results)
    return (*outs[:4], outs[4].reshape(3, 2 * part, width), outs[5].reshape(2 * part, width),
            outs[6].reshape(2, 2 * part, width), outs[7].reshape(2 * part, width))


def solution(mesh):
    rows = P(("region", "feat"), None)
    blocks = (P(None, "feat", None), P("feat", None), P(None, "feat", None), P("feat", None))
    in_specs = (rows, rows, P("region"), P("region"), P("region", None, None), *blocks, P("feat"), P("feat"), rows, rows)
    sizes = (mesh.shape["region"], mesh.shape["feat"])
    return jax.shard_map(lambda *args: shards(sizes, *args), mesh=mesh, in_specs=in_specs,
                         out_specs=(rows, rows, rows, rows, *blocks), check_vma=False)
```

```python
import jax
import jax.numpy as jnp
from jax import lax
from jax.experimental import pallas as pl
from jax.experimental.pallas import tpu as pltpu
from jax.sharding import PartitionSpec as P

MESH = pl.DeviceIdType.MESH
BF16, F32 = jnp.bfloat16, jnp.float32
EPSILON = 1e-05
SIDE = 4
EDGE_W, NODE_W = (0, 4), (4, 3)
VMEM_LIMIT = 44 * 2**20


def dot(a, b, da, db):
    return lax.dot_general(a, b, (((da,), (db,)), ((), ())), preferred_element_type=F32)


def mm(a, b):
    return dot(a, b, 1, 0)


def mm_back(a, b):
    return dot(a, b, 1, 1)


def mm_t(a, b):
    return dot(a, b, 0, 0)


def sigmoid(v):
    return 1.0 / (1.0 + jnp.exp(-v))


def layer_norm(m):
    width = m.shape[1]
    mean = jnp.sum(m, axis=1, keepdims=True) / width
    var = jnp.sum(m * m, axis=1, keepdims=True) / width - mean * mean
    inverse = lax.rsqrt(var + EPSILON)
    return (m - mean) * inverse, inverse


def layer_norm_back(cot, normed, inverse, gain):
    width = cot.shape[1]
    s = cot * gain
    first = jnp.sum(s, axis=1, keepdims=True) / width
    second = jnp.sum(s * normed, axis=1, keepdims=True) / width
    return (inverse * (s - first - normed * second)).astype(BF16)


def iota(shape, dim):
    return lax.broadcasted_iota(jnp.int32, shape, dim)


def rows_equal(count, index, base=0):
    rows = iota((count, index.shape[1]), 0) + base
    return jnp.where(rows == index, 1.0, 0.0).astype(BF16)


def flat(blocks, pick, mine):
    wide = lax.dot_general(blocks, jnp.where(pick, 1.0, 0.0), (((1,), (0,)), ((), ())),
                           precision=lax.Precision.HIGHEST, preferred_element_type=F32)
    return jnp.sum(jnp.where(mine, wide, 0.0), axis=0, keepdims=True)


def own_slice(ref, f, edges):
    lines = 2 * edges // 128
    start = lax.div(f, 2) * lines
    two = jnp.concatenate([ref[start + i] for i in range(lines)], axis=1)
    return jnp.where(lax.rem(f, 2) == 1, two[:, edges:], two[:, :edges])


def kernel(regions, feats, scales, fetches,
           node, edge, recv_all, send_all, listed_at, wei, weo, wni, wno, egain, ngain, ncot, ecot,
           node_new, edge_new, node_grad, edge_grad, wgrad,
           nodes, gains, w, outgo, income, pre, normed, srows, rrows, hid, emg,
           pool_s, pool_r, npg, ng_s, ng_r, rem_s, rem_r,
           dw, pe_s, pe_r, pn_s, pn_r, re_s, re_r, rn_s, rn_r, qe_s, qe_r, qn_s, qn_r,
           ze_s, ze_r, zn_s, zn_r, be, bn, ssem, rsem):
    g, f = lax.axis_index("region"), lax.axis_index("feat")
    c, z = lax.rem(g, 2), lax.div(g, 2)
    y, x = lax.div(f, SIDE), lax.rem(f, SIDE)
    sibling = g + 1 - 2 * c
    first = c == 0
    a = jnp.where(first, x, y)
    b = jnp.where(first, y, x)
    chips = regions // 2
    per, width = node.shape
    edges = edge.shape[0]
    count = per * feats
    slots = income.shape[1]
    far = regions * slots

    def feat_at(a_, b_):
        return jnp.where(first, SIDE * b_ + a_, SIDE * a_ + b_)

    def send(src, dst, k, region, feat):
        return pltpu.make_async_remote_copy(
            src_ref=src, dst_ref=dst, send_sem=ssem.at[k], recv_sem=rsem.at[k],
            device_id=(region, feat), device_id_type=MESH)

    def to_plane(src_of, dst, k):
        def body(j, carry):
            t = lax.rem(f + j, feats)
            send(src_of(t), dst.at[f], k, g, t).start()
            return carry
        lax.fori_loop(1, feats, body, 0)

    def to_line(src_of, dst, k):
        def body(j, carry):
            t = lax.rem(g + j, regions)
            send(src_of(t), dst.at[g], k, t, f).start()
            return carry
        lax.fori_loop(1, regions, body, 0)

    def settle(view, k):
        send(view, view, k, g, f).wait()

    def settle_slots(buffer, k):
        settle(buffer.at[pl.ds(0, buffer.shape[0] - 1)], k)

    barrier = pltpu.get_barrier_semaphore()

    def greet(j, carry):
        pl.semaphore_signal(barrier, inc=1, device_id=(g, lax.rem(f + j, feats)), device_id_type=MESH)
        pl.semaphore_signal(barrier, inc=1, device_id=(lax.rem(g + j, regions), f), device_id_type=MESH)
        return carry
    lax.fori_loop(1, feats, greet, 0)
    for fetch in fetches:
        fetch.wait()

    portion = egain.shape[1]
    gains[f] = jnp.concatenate([egain[...], ngain[...], jnp.zeros((1, gains.shape[2] - 2 * portion), F32)], axis=1)
    nodes[f] = node[...]
    for k in range(3):
        w[k, y, x, c] = wei[k, c]
    w[3, y, x, c] = weo[c]
    for k in range(2):
        w[4 + k, y, x, c] = wni[k, c]
    w[6, y, x, c] = wno[c]
    income[g] = jnp.zeros(income.shape[1:], BF16)
    rem_r[g] = jnp.zeros(rem_r.shape[1:], BF16)
    recv_at = own_slice(recv_all, f, edges)
    send_at = own_slice(send_all, f, edges)
    grid = (regions, far)
    listed = flat(listed_at[0].astype(F32), lax.rem(iota((slots, far), 1), slots) == iota((slots, far), 0),
                  lax.div(iota(grid, 1), slots) == iota(grid, 0))
    asked = jnp.where(iota((count, far), 0).astype(F32) == listed, 1.0, 0.0).astype(BF16)
    into = rows_equal(count, recv_at)
    near = rows_equal(count, send_at)
    away = rows_equal(far, send_at, count)
    pl.semaphore_wait(barrier, feats - 1 + regions - 1)

    def weights_first(group, k):
        part = w.at[pl.ds(*group), y, x, c]
        for d in range(1, SIDE):
            send(part, part, k, g, feat_at(lax.rem(a + d, SIDE), b)).start()

    def bundle(group, b_, act):
        ks = pl.ds(*group)

        @pl.when(first)
        def _():
            act(w.at[ks, b_, :, 0])

        @pl.when(c == 1)
        def _():
            act(w.at[ks, :, b_, 1])

    def weights_second(group, k, k2):
        settle(w.at[pl.ds(*group), 0, pl.ds(0, SIDE - 1), 0], k)

        def act(part):
            for d in (2, 1, 3):
                send(part, part, k2 + d, g, feat_at(a, lax.rem(b + d, SIDE))).start()
            send(part, part, k2, sibling, f).start()
        bundle(group, b, act)

    def weights_pass(group, k2, d):
        settle(w.at[pl.ds(*group), 0, :, 0], k2 + d)
        bundle(group, lax.rem(b - d + SIDE, SIDE), lambda part: send(part, part, k2, sibling, f).start())

    def weights_end(group, k2):
        settle(w.at[pl.ds(*group), :, :, 0], k2)

    weights_first(EDGE_W, 2)
    to_plane(lambda t: node, nodes, 0)
    weights_first(NODE_W, 3)
    to_plane(lambda t: gains.at[f], gains, 1)
    weights_second(EDGE_W, 2, 5)
    settle_slots(nodes, 0)
    table = nodes[...].reshape(count, width)
    outgo[...] = mm_t(asked, table).astype(BF16).reshape(outgo.shape)
    to_line(lambda t: outgo.at[t], income, 4)
    weights_second(NODE_W, 3, 9)
    rrows[...] = mm_t(into, table).astype(BF16)
    near_rows = mm_t(near, table)
    settle_slots(gains, 1)
    packed = gains[...].reshape(feats, gains.shape[2])
    shape, wide = (gains.shape[2], 2 * width), (feats, 2 * width)
    lanes = iota(shape, 1)
    gain = flat(packed, lax.rem(lanes, portion) + portion * lax.div(lanes, width) == iota(shape, 0),
                lax.div(lax.rem(iota(wide, 1), width), portion) == iota(wide, 0))
    edge_gain, node_gain = gain[:, :width], gain[:, width:]
    weights_pass(EDGE_W, 5, 1)
    weights_pass(EDGE_W, 5, 3)
    weights_pass(EDGE_W, 5, 2)
    settle_slots(income, 4)
    srows[...] = (near_rows + mm_t(away, income[...].reshape(far, width))).astype(BF16)
    weights_end(EDGE_W, 5)

    def weight(k):
        return w[k].reshape(width, width)

    pre[...] = mm(edge[...], weight(0)) + mm(srows[...], weight(1)) + mm(rrows[...], weight(2))
    hid[...] = (pre[...] * sigmoid(pre[...])).astype(BF16)
    edge_normed, edge_inverse = layer_norm(mm(hid[...], weight(3)))
    normed[...] = edge_normed
    fresh = (edge[...].astype(F32) + edge_normed * edge_gain).astype(BF16)
    edge_new[...] = fresh
    pool_s[...] = mm(into, fresh).astype(BF16).reshape(pool_s.shape)
    pool_r[f] = pool_s[f]
    to_plane(lambda t: pool_s.at[t], pool_r, 13)
    for d in (1, 3, 2):
        weights_pass(NODE_W, 9, d)
    gate = sigmoid(pre[...])
    pre[...] = gate * (1.0 + pre[...] * (1.0 - gate))
    weights_end(NODE_W, 9)
    lat = node[...]
    node_base = mm(lat, weight(4))
    settle_slots(pool_r, 13)

    pooled = jnp.sum(pool_r[...].astype(F32), axis=0).astype(BF16)
    node_pre = node_base + mm(pooled, weight(5))
    gate = sigmoid(node_pre)
    node_hid = (node_pre * gate).astype(BF16)
    node_normed, node_inverse = layer_norm(mm(node_hid, weight(6)))
    node_new[...] = (lat.astype(F32) + node_normed * node_gain).astype(BF16)
    nmg = layer_norm_back(ncot[...].astype(F32), node_normed, node_inverse, node_gain)
    slope = gate * (1.0 + node_pre * (1.0 - gate))
    own_npg = (mm_back(nmg, weight(6)) * slope).astype(BF16)
    npg[f] = own_npg
    to_plane(lambda t: npg.at[f], npg, 14)

    def trade(k, product, out, back, s):
        dw[k] = product.reshape(dw.shape[1:])
        out[...] = dw[k, :, 1 - c].astype(BF16)
        send(out, back, s, sibling, f).start()

    def along_a(k, i, back, stage, landed, s, s2):
        settle(back, s)

        def body(j, carry):
            a_, b_ = lax.div(j, SIDE), lax.rem(j, SIDE)
            at = feat_at(a_, b_)
            stage[a_, i, b_] = (dw[k, at, c] + back[at].astype(F32)).astype(BF16)
            return carry
        lax.fori_loop(0, feats, body, 0, unroll=True)
        landed[a, i] = stage[a, i]
        for d in (2, 1, 3):
            a_ = lax.rem(a + d, SIDE)
            send(stage.at[a_, i], landed.at[a, i], s2, g, feat_at(a_, b)).start()

    def along_b(landed, stage, landed2, k2, k3):
        settle_slots(landed, k2)

        def body(b_, carry):
            stage[b_] = jnp.sum(landed[:, :, b_].astype(F32), axis=0).astype(BF16)
            return carry
        lax.fori_loop(0, SIDE, body, 0)
        landed2[b] = stage[b]
        for d in range(1, SIDE):
            b_ = lax.rem(b + d, SIDE)
            send(stage.at[b_], landed2.at[b], k3, g, feat_at(a, b_)).start()

    def along_z(landed, stage, landed2, k3, k4):
        settle_slots(landed, k3)
        whole = jnp.sum(landed[...].astype(F32), axis=0).astype(BF16)
        rows = stage.shape[1]
        pieces = whole.reshape(whole.shape[0] * whole.shape[1] // rows, rows, width)
        stage[pl.ds(0, pieces.shape[0])] = pieces
        if pieces.shape[0] < chips:
            stage[pl.ds(pieces.shape[0], chips - pieces.shape[0])] = jnp.zeros(
                (chips - pieces.shape[0], rows, width), BF16)
        landed2[z] = stage[z]
        for d in range(1, chips):
            z_ = lax.rem(z + d, chips)
            send(stage.at[z_], landed2.at[z], k4, 2 * z_ + c, f).start()

    def to_all(landed, whole, k4, k5, scale):
        settle_slots(landed, k4)
        whole[g] = (jnp.sum(landed[...].astype(F32), axis=0) * scale).astype(BF16)
        to_line(lambda t: whole.at[g], whole, k5)

    def finish(group, whole, k5):
        settle_slots(whole, k5)
        start, n = group
        rows = whole.shape[1]
        halves = wgrad.shape[2] // rows
        for i in range(n):
            for c_ in range(2):
                for h in range(halves):
                    wgrad[start + i, c_, pl.ds(h * rows, rows)] = whole[2 * (halves * i + h) + c_].astype(F32)

    node_sides = ((lat, own_npg), (pooled, own_npg), (node_hid, nmg))
    for i in range(3):
        trade(4 + i, mm_t(*node_sides[i]), pn_s.at[i], pn_r.at[i], 29 + i)
    direct = ncot[...].astype(F32) + mm_back(own_npg, weight(4))
    for i in range(3):
        along_a(4 + i, i, pn_r.at[i], rn_s, rn_r, 29 + i, 16)
    settle_slots(npg, 14)

    reached = mm_t(into, npg[...].reshape(count, width)).astype(BF16)
    total = ecot[...].astype(F32) + mm_back(reached, weight(5))
    emg[...] = layer_norm_back(total, normed[...], edge_inverse, edge_gain)
    pre_grad = (mm_back(emg[...], weight(3)) * pre[...]).astype(BF16)
    trade(3, mm_t(hid[...], emg[...]), pe_s.at[3], pe_r.at[3], 35)
    from_send = mm_back(pre_grad, weight(1)).astype(BF16)
    rem_s[...] = mm(away, from_send).astype(BF16).reshape(rem_s.shape)
    to_line(lambda t: rem_s.at[t], rem_r, 18)
    trade(0, mm_t(edge[...], pre_grad), pe_s.at[0], pe_r.at[0], 32)
    along_a(3, 3, pe_r.at[3], re_s, re_r, 35, 19)
    trade(1, mm_t(srows[...], pre_grad), pe_s.at[1], pe_r.at[1], 33)
    along_a(0, 0, pe_r.at[0], re_s, re_r, 32, 19)
    trade(2, mm_t(rrows[...], pre_grad), pe_s.at[2], pe_r.at[2], 34)
    along_a(1, 1, pe_r.at[1], re_s, re_r, 33, 19)
    along_a(2, 2, pe_r.at[2], re_s, re_r, 34, 19)
    along_b(rn_r, qn_s, qn_r, 16, 20)
    from_recv = mm_back(pre_grad, weight(2)).astype(BF16)
    ng = mm(near, from_send) + mm(into, from_recv)
    edge_grad[...] = total + mm_back(pre_grad, weight(0))
    along_b(re_r, qe_s, qe_r, 19, 24)

    settle_slots(rem_r, 18)
    ng = ng + mm(asked, rem_r[...].reshape(far, width))
    ng_s[...] = ng.astype(BF16).reshape(ng_s.shape)
    ng_r[f] = ng_s[f]
    along_z(qn_r, zn_s, zn_r, 20, 23)
    along_z(qe_r, ze_s, ze_r, 24, 26)
    to_plane(lambda t: ng_s.at[t], ng_r, 21)
    to_all(zn_r, bn, 23, 27, scales[1])
    to_all(ze_r, be, 26, 28, scales[0])
    settle_slots(ng_r, 21)
    node_grad[...] = direct + jnp.sum(ng_r[...].astype(F32), axis=0)
    finish(NODE_W, bn, 27)
    finish(EDGE_W, be, 28)


def hand_on(*refs):
    sources, outs, out = refs[:5], refs[5:13], refs[13]
    grads = sources[4]
    views = [*sources[:4], grads.at[pl.ds(0, 3)], grads.at[3], grads.at[pl.ds(4, 2)], grads.at[6]]
    copies = [pltpu.make_async_copy(v, o, out.at[i]) for i, (v, o) in enumerate(zip(views, outs))]
    for copy in copies:
        copy.start()
    for copy in copies:
        copy.wait()


def shards(sizes, node_lat, edge_lat, receiver_row, sender_slot, send_rows, w_edge_in, w_edge_out, w_node_in,
           w_node_out, edge_gain, node_gain, node_cot, edge_cot):
    regions, feats = sizes
    per, width = node_lat.shape
    edges = edge_lat.shape[0]
    slots = send_rows.shape[2]
    part = width // feats // 2
    lines = (edges * feats // 128, 1, 128)
    scales = (1.0 / float(edges * feats * regions) ** 0.5, 1.0 / float(per * feats * regions) ** 0.5)
    ne, nn = EDGE_W[1], NODE_W[1]
    piece = ne * part // (regions // 2)

    def v(dtype, *shape):
        return pltpu.VMEM(shape, dtype)

    nodes_like = (feats, per, width)
    line_like = (regions, slots, width)

    def pair(dtype, *shape):
        return [v(dtype, *shape)] * 2

    scratch = [
        v(BF16, *nodes_like), v(F32, feats, 1, 128), v(BF16, ne + nn, SIDE, SIDE, 2, part, width),
        *pair(BF16, *line_like),
        *pair(F32, edges, width),
        *[v(BF16, edges, width)] * 4,
        *pair(BF16, *nodes_like), v(BF16, *nodes_like), *pair(BF16, *nodes_like), *pair(BF16, *line_like),
        v(F32, ne + nn, feats, 2, part, width),
        *pair(BF16, ne, feats, part, width), *pair(BF16, nn, feats, part, width),
        *pair(BF16, SIDE, ne, SIDE, part, width), *pair(BF16, SIDE, nn, SIDE, part, width),
        *pair(BF16, SIDE, ne, part, width), *pair(BF16, SIDE, nn, part, width),
        *pair(BF16, regions // 2, piece, width), *pair(BF16, regions // 2, piece, width),
        *pair(BF16, regions, piece, width),
        pltpu.SemaphoreType.DMA((36,)), pltpu.SemaphoreType.DMA((36,)),
    ]

    args = (node_lat, edge_lat, receiver_row.reshape(lines), sender_slot.reshape(lines), send_rows,
            w_edge_in.reshape(3, 2, part, width), w_edge_out.reshape(2, part, width),
            w_node_in.reshape(2, 2, part, width), w_node_out.reshape(2, part, width),
            edge_gain[None], node_gain[None], node_cot, edge_cot)
    n = len(args)
    scratch += [*[v(x.dtype, *x.shape) for x in args], pltpu.SemaphoreType.DMA((n,))]

    def body(*refs):
        sources, rest = refs[:n], refs[n:]
        held, sem = rest[-n - 1:-1], rest[-1]
        fetches = [pltpu.make_async_copy(s, h, sem.at[i]) for i, (s, h) in enumerate(zip(sources, held))]
        for fetch in fetches:
            fetch.start()
        kernel(regions, feats, scales, fetches, *held, *rest[:-n - 1])

    vmem = pl.BlockSpec(memory_space=pltpu.VMEM)
    kinds = [((per, width), BF16), ((edges, width), BF16), ((per, width), F32), ((edges, width), F32)]
    blocks = [(3, 2, part, width), (2, part, width), (2, 2, part, width), (2, part, width)]
    results = pl.pallas_call(
        body,
        name="layer",
        out_shape=[jax.ShapeDtypeStruct(*k) for k in (*kinds, ((ne + nn, 2, part, width), F32))],
        in_specs=[pl.BlockSpec(memory_space=pltpu.HBM)] * n,
        out_specs=[vmem] * 5,
        scratch_shapes=scratch,
        compiler_params=pltpu.CompilerParams(
            collective_id=0, has_side_effects=True, vmem_limit_bytes=VMEM_LIMIT),
    )(*[pltpu.with_memory_space_constraint(x, pltpu.HBM) for x in args])
    kinds += [(s, F32) for s in blocks]
    outs = pl.pallas_call(
        hand_on,
        name="hand_on",
        out_shape=[jax.ShapeDtypeStruct(*k) for k in kinds],
        in_specs=[vmem] * 5,
        out_specs=[pl.BlockSpec(memory_space=pltpu.HBM)] * 8,
        scratch_shapes=[pltpu.SemaphoreType.DMA((8,))],
        compiler_params=pltpu.CompilerParams(vmem_limit_bytes=8 * 2**20),
    )(*results)
    return (*outs[:4], outs[4].reshape(3, 2 * part, width), outs[5].reshape(2 * part, width),
            outs[6].reshape(2, 2 * part, width), outs[7].reshape(2 * part, width))


def solution(mesh):
    rows = P(("region", "feat"), None)
    blocks = (P(None, "feat", None), P("feat", None), P(None, "feat", None), P("feat", None))
    in_specs = (rows, rows, P("region"), P("region"), P("region", None, None), *blocks, P("feat"), P("feat"), rows, rows)
    sizes = (mesh.shape["region"], mesh.shape["feat"])
    return jax.shard_map(lambda *args: shards(sizes, *args), mesh=mesh, in_specs=in_specs,
                         out_specs=(rows, rows, rows, rows, *blocks), check_vma=False)
```

```python
import jax
import jax.numpy as jnp
from jax import lax
from jax.experimental import pallas as pl
from jax.experimental.pallas import tpu as pltpu
from jax.sharding import PartitionSpec as P

MESH = pl.DeviceIdType.MESH
BF16, F32 = jnp.bfloat16, jnp.float32
EPSILON = 1e-05
SIDE = 4
EDGE_W, NODE_W = (0, 4), (4, 3)
VMEM_LIMIT = 44 * 2**20


def hops(d, n):
    return min(d, n - d)


def far_first(n):
    return sorted(range(1, n), key=lambda d: -hops(d, n))


PLANE_STEPS = sorted(((dy, dx) for dy in range(SIDE) for dx in range(SIDE) if dy or dx),
                     key=lambda s: -hops(s[0], SIDE) - hops(s[1], SIDE))


def dot(a, b, da, db):
    return lax.dot_general(a, b, (((da,), (db,)), ((), ())), preferred_element_type=F32)


def mm(a, b):
    return dot(a, b, 1, 0)


def mm_back(a, b):
    return dot(a, b, 1, 1)


def mm_t(a, b):
    return dot(a, b, 0, 0)


def sigmoid(v):
    return 1.0 / (1.0 + jnp.exp(-v))


def layer_norm(m):
    width = m.shape[1]
    mean = jnp.sum(m, axis=1, keepdims=True) / width
    var = jnp.sum(m * m, axis=1, keepdims=True) / width - mean * mean
    inverse = lax.rsqrt(var + EPSILON)
    return (m - mean) * inverse, inverse


def layer_norm_back(cot, normed, inverse, gain):
    width = cot.shape[1]
    s = cot * gain
    first = jnp.sum(s, axis=1, keepdims=True) / width
    second = jnp.sum(s * normed, axis=1, keepdims=True) / width
    return (inverse * (s - first - normed * second)).astype(BF16)


def iota(shape, dim):
    return lax.broadcasted_iota(jnp.int32, shape, dim)


def rows_equal(count, index, base=0):
    rows = iota((count, index.shape[1]), 0) + base
    return jnp.where(rows == index, 1.0, 0.0).astype(BF16)


def flat(blocks, pick, mine):
    wide = lax.dot_general(blocks, jnp.where(pick, 1.0, 0.0), (((1,), (0,)), ((), ())),
                           precision=lax.Precision.HIGHEST, preferred_element_type=F32)
    return jnp.sum(jnp.where(mine, wide, 0.0), axis=0, keepdims=True)


def own_slice(ref, f, edges):
    lines = 2 * edges // 128
    start = lax.div(f, 2) * lines
    two = jnp.concatenate([ref[start + i] for i in range(lines)], axis=1)
    return jnp.where(lax.rem(f, 2) == 1, two[:, edges:], two[:, :edges])


def kernel(regions, feats, scales, fetches,
           node, edge, recv_all, send_all, listed_at, wei, weo, wni, wno, egain, ngain, ncot, ecot,
           node_new, edge_new, node_grad, edge_grad, wgrad,
           nodes, gains, w, outgo, income, pre, normed, srows, rrows, hid, emg,
           pool_s, pool_r, npg, ng_s, ng_r, rem_s, rem_r,
           dw, pe_s, pe_r, pn_s, pn_r, re_s, re_r, rn_s, rn_r, qe_s, qe_r, qn_s, qn_r,
           ze_s, ze_r, zn_s, zn_r, be, bn, ssem, rsem):
    g, f = lax.axis_index("region"), lax.axis_index("feat")
    c, z = lax.rem(g, 2), lax.div(g, 2)
    y, x = lax.div(f, SIDE), lax.rem(f, SIDE)
    sibling = g + 1 - 2 * c
    first = c == 0
    a = jnp.where(first, x, y)
    b = jnp.where(first, y, x)
    chips = regions // 2
    per, width = node.shape
    edges = edge.shape[0]
    count = per * feats
    slots = income.shape[1]
    far = regions * slots

    def feat_at(a_, b_):
        return jnp.where(first, SIDE * b_ + a_, SIDE * a_ + b_)

    def send(src, dst, k, region, feat):
        return pltpu.make_async_remote_copy(
            src_ref=src, dst_ref=dst, send_sem=ssem.at[k], recv_sem=rsem.at[k],
            device_id=(region, feat), device_id_type=MESH)

    def to_plane(src_of, dst, k):
        for dy, dx in PLANE_STEPS:
            t = SIDE * lax.rem(y + dy, SIDE) + lax.rem(x + dx, SIDE)
            send(src_of(t), dst.at[f], k, g, t).start()

    def to_line(src_of, dst, k):
        for j in far_first(regions):
            t = lax.rem(g + j, regions)
            send(src_of(t), dst.at[g], k, t, f).start()

    def settle(view, k):
        send(view, view, k, g, f).wait()

    def settle_slots(buffer, k):
        settle(buffer.at[pl.ds(0, buffer.shape[0] - 1)], k)

    barrier = pltpu.get_barrier_semaphore()

    for (dy, dx), j in zip(PLANE_STEPS, far_first(regions)):
        t = SIDE * lax.rem(y + dy, SIDE) + lax.rem(x + dx, SIDE)
        pl.semaphore_signal(barrier, inc=1, device_id=(g, t), device_id_type=MESH)
        pl.semaphore_signal(barrier, inc=1, device_id=(lax.rem(g + j, regions), f), device_id_type=MESH)
    for fetch in fetches:
        fetch.wait()

    portion = egain.shape[1]
    gains[f] = jnp.concatenate([egain[...], ngain[...], jnp.zeros((1, gains.shape[2] - 2 * portion), F32)], axis=1)
    nodes[y, x] = node[...]
    for k in range(3):
        w[k, y, x, c] = wei[k, c]
    w[3, y, x, c] = weo[c]
    for k in range(2):
        w[4 + k, y, x, c] = wni[k, c]
    w[6, y, x, c] = wno[c]
    income[g] = jnp.zeros(income.shape[1:], BF16)
    rem_r[g] = jnp.zeros(rem_r.shape[1:], BF16)
    recv_at = own_slice(recv_all, f, edges)
    send_at = own_slice(send_all, f, edges)
    grid = (regions, far)
    listed = flat(listed_at[0].astype(F32), lax.rem(iota((slots, far), 1), slots) == iota((slots, far), 0),
                  lax.div(iota(grid, 1), slots) == iota(grid, 0))
    asked = jnp.where(iota((count, far), 0).astype(F32) == listed, 1.0, 0.0).astype(BF16)
    into = rows_equal(count, recv_at)
    near = rows_equal(count, send_at)
    away = rows_equal(far, send_at, count)
    pl.semaphore_wait(barrier, feats - 1 + regions - 1)

    def weights_first(group, k):
        part = w.at[pl.ds(*group), y, x, c]
        for d in range(1, SIDE):
            send(part, part, k, g, feat_at(lax.rem(a + d, SIDE), b)).start()

    def bundle(group, b_, act):
        ks = pl.ds(*group)

        @pl.when(first)
        def _():
            act(w.at[ks, b_, :, 0])

        @pl.when(c == 1)
        def _():
            act(w.at[ks, :, b_, 1])

    def weights_second(group, k, k2):
        settle(w.at[pl.ds(*group), 0, pl.ds(0, SIDE - 1), 0], k)

        def act(part):
            for d in (1, 3):
                send(part, part, k2 + d, g, feat_at(a, lax.rem(b + d, SIDE))).start()
            send(part, part, k2, sibling, f).start()
        bundle(group, b, act)

    def weights_pass(group, k2, d):
        settle(w.at[pl.ds(*group), 0, :, 0], k2 + d)

        def act(part):
            send(part, part, k2, sibling, f).start()
            if d != 2:
                half = part.at[:, :, pl.ds(0 if d == 1 else part.shape[2] // 2, part.shape[2] // 2)]
                send(half, half, k2 + 2, g, feat_at(a, lax.rem(b + d, SIDE))).start()
        bundle(group, lax.rem(b - d + SIDE, SIDE), act)

    def weights_end(group, k2):
        settle(w.at[pl.ds(*group), :, :, 0], k2)

    def nodes_second(part):
        for d in (2, 1, 3):
            send(part, part, 36, g, feat_at(a, lax.rem(b + d, SIDE))).start()

    for d in range(1, SIDE):
        send(node, nodes.at[y, x], 0, g, feat_at(lax.rem(a + d, SIDE), b)).start()
    weights_first(EDGE_W, 2)
    weights_first(NODE_W, 3)
    to_plane(lambda t: gains.at[f], gains, 1)
    settle(nodes.at[0, pl.ds(0, SIDE - 1)], 0)

    @pl.when(first)
    def _():
        nodes_second(nodes.at[y])

    @pl.when(c == 1)
    def _():
        nodes_second(nodes.at[:, x])

    weights_second(EDGE_W, 2, 5)
    weights_second(NODE_W, 3, 9)
    settle_slots(nodes, 36)
    table = nodes[...].reshape(count, width)
    outgo[...] = mm_t(asked, table).astype(BF16).reshape(outgo.shape)
    to_line(lambda t: outgo.at[t], income, 4)
    rrows[...] = mm_t(into, table).astype(BF16)
    near_rows = mm_t(near, table)
    settle_slots(gains, 1)
    packed = gains[...].reshape(feats, gains.shape[2])
    shape, wide = (gains.shape[2], 2 * width), (feats, 2 * width)
    lanes = iota(shape, 1)
    gain = flat(packed, lax.rem(lanes, portion) + portion * lax.div(lanes, width) == iota(shape, 0),
                lax.div(lax.rem(iota(wide, 1), width), portion) == iota(wide, 0))
    edge_gain, node_gain = gain[:, :width], gain[:, width:]
    for d in (1, 3, 2):
        weights_pass(EDGE_W, 5, d)
    weights_pass(NODE_W, 9, 1)
    weights_pass(NODE_W, 9, 3)
    settle_slots(income, 4)
    srows[...] = (near_rows + mm_t(away, income[...].reshape(far, width))).astype(BF16)
    weights_end(EDGE_W, 5)

    def weight(k):
        return w[k].reshape(width, width)

    pre[...] = mm(edge[...], weight(0)) + mm(srows[...], weight(1)) + mm(rrows[...], weight(2))
    hid[...] = (pre[...] * sigmoid(pre[...])).astype(BF16)
    edge_normed, edge_inverse = layer_norm(mm(hid[...], weight(3)))
    normed[...] = edge_normed
    fresh = (edge[...].astype(F32) + edge_normed * edge_gain).astype(BF16)
    edge_new[...] = fresh
    pool_s[...] = mm(into, fresh).astype(BF16).reshape(pool_s.shape)
    pool_r[f] = pool_s[f]
    to_plane(lambda t: pool_s.at[t], pool_r, 13)
    weights_pass(NODE_W, 9, 2)
    gate = sigmoid(pre[...])
    pre[...] = gate * (1.0 + pre[...] * (1.0 - gate))
    weights_end(NODE_W, 9)
    lat = node[...]
    node_base = mm(lat, weight(4))
    settle_slots(pool_r, 13)

    pooled = jnp.sum(pool_r[...].astype(F32), axis=0).astype(BF16)
    node_pre = node_base + mm(pooled, weight(5))
    gate = sigmoid(node_pre)
    node_hid = (node_pre * gate).astype(BF16)
    node_normed, node_inverse = layer_norm(mm(node_hid, weight(6)))
    node_new[...] = (lat.astype(F32) + node_normed * node_gain).astype(BF16)
    nmg = layer_norm_back(ncot[...].astype(F32), node_normed, node_inverse, node_gain)
    slope = gate * (1.0 + node_pre * (1.0 - gate))
    own_npg = (mm_back(nmg, weight(6)) * slope).astype(BF16)
    npg[f] = own_npg
    to_plane(lambda t: npg.at[f], npg, 14)

    def trade(k, product, out, back, s):
        dw[k] = product.reshape(dw.shape[1:])
        out[...] = dw[k, :, 1 - c].astype(BF16)
        send(out, back, s, sibling, f).start()

    def along_a(k, i, back, stage, landed, s, s2):
        settle(back, s)

        def body(j, carry):
            a_, b_ = lax.div(j, SIDE), lax.rem(j, SIDE)
            at = feat_at(a_, b_)
            stage[a_, i, b_] = (dw[k, at, c] + back[at].astype(F32)).astype(BF16)
            return carry
        lax.fori_loop(0, feats, body, 0, unroll=True)
        landed[a, i] = stage[a, i]
        for d in (2, 1, 3):
            a_ = lax.rem(a + d, SIDE)
            send(stage.at[a_, i], landed.at[a, i], s2, g, feat_at(a_, b)).start()

    def along_b(landed, stage, landed2, k2, k3):
        settle_slots(landed, k2)

        def body(b_, carry):
            stage[b_] = jnp.sum(landed[:, :, b_].astype(F32), axis=0).astype(BF16)
            return carry
        lax.fori_loop(0, SIDE, body, 0)
        landed2[b] = stage[b]
        for d in range(1, SIDE):
            b_ = lax.rem(b + d, SIDE)
            send(stage.at[b_], landed2.at[b], k3, g, feat_at(a, b_)).start()

    def along_z(landed, stage, landed2, k3, k4):
        settle_slots(landed, k3)
        whole = jnp.sum(landed[...].astype(F32), axis=0).astype(BF16)
        rows = stage.shape[1]
        pieces = whole.reshape(whole.shape[0] * whole.shape[1] // rows, rows, width)
        stage[pl.ds(0, pieces.shape[0])] = pieces
        if pieces.shape[0] < chips:
            stage[pl.ds(pieces.shape[0], chips - pieces.shape[0])] = jnp.zeros(
                (chips - pieces.shape[0], rows, width), BF16)
        landed2[z] = stage[z]
        for d in far_first(chips):
            z_ = lax.rem(z + d, chips)
            send(stage.at[z_], landed2.at[z], k4, 2 * z_ + c, f).start()

    def to_all(landed, whole, k4, k5, scale):
        settle_slots(landed, k4)
        whole[g] = (jnp.sum(landed[...].astype(F32), axis=0) * scale).astype(BF16)
        to_line(lambda t: whole.at[g], whole, k5)

    def finish(group, whole, k5):
        settle_slots(whole, k5)
        start, n = group
        rows = whole.shape[1]
        halves = wgrad.shape[2] // rows
        for i in range(n):
            for c_ in range(2):
                for h in range(halves):
                    wgrad[start + i, c_, pl.ds(h * rows, rows)] = whole[2 * (halves * i + h) + c_].astype(F32)

    node_sides = ((lat, own_npg), (pooled, own_npg), (node_hid, nmg))
    for i in range(3):
        trade(4 + i, mm_t(*node_sides[i]), pn_s.at[i], pn_r.at[i], 29 + i)
    direct = ncot[...].astype(F32) + mm_back(own_npg, weight(4))
    for i in range(3):
        along_a(4 + i, i, pn_r.at[i], rn_s, rn_r, 29 + i, 16)
    settle_slots(npg, 14)

    reached = mm_t(into, npg[...].reshape(count, width)).astype(BF16)
    total = ecot[...].astype(F32) + mm_back(reached, weight(5))
    emg[...] = layer_norm_back(total, normed[...], edge_inverse, edge_gain)
    pre_grad = (mm_back(emg[...], weight(3)) * pre[...]).astype(BF16)
    trade(3, mm_t(hid[...], emg[...]), pe_s.at[3], pe_r.at[3], 35)
    from_send = mm_back(pre_grad, weight(1)).astype(BF16)
    rem_s[...] = mm(away, from_send).astype(BF16).reshape(rem_s.shape)
    to_line(lambda t: rem_s.at[t], rem_r, 18)
    trade(0, mm_t(edge[...], pre_grad), pe_s.at[0], pe_r.at[0], 32)
    along_a(3, 3, pe_r.at[3], re_s, re_r, 35, 19)
    trade(1, mm_t(srows[...], pre_grad), pe_s.at[1], pe_r.at[1], 33)
    along_a(0, 0, pe_r.at[0], re_s, re_r, 32, 19)
    trade(2, mm_t(rrows[...], pre_grad), pe_s.at[2], pe_r.at[2], 34)
    along_a(1, 1, pe_r.at[1], re_s, re_r, 33, 19)
    along_a(2, 2, pe_r.at[2], re_s, re_r, 34, 19)
    along_b(rn_r, qn_s, qn_r, 16, 20)
    from_recv = mm_back(pre_grad, weight(2)).astype(BF16)
    ng = mm(near, from_send) + mm(into, from_recv)
    edge_grad[...] = total + mm_back(pre_grad, weight(0))
    along_b(re_r, qe_s, qe_r, 19, 24)

    settle_slots(rem_r, 18)
    ng = ng + mm(asked, rem_r[...].reshape(far, width))
    ng_s[...] = ng.astype(BF16).reshape(ng_s.shape)
    ng_r[f] = ng_s[f]
    along_z(qn_r, zn_s, zn_r, 20, 23)
    along_z(qe_r, ze_s, ze_r, 24, 26)
    to_plane(lambda t: ng_s.at[t], ng_r, 21)
    to_all(zn_r, bn, 23, 27, scales[1])
    to_all(ze_r, be, 26, 28, scales[0])
    settle_slots(ng_r, 21)
    node_grad[...] = direct + jnp.sum(ng_r[...].astype(F32), axis=0)
    finish(NODE_W, bn, 27)
    finish(EDGE_W, be, 28)


def hand_on(*refs):
    sources, outs, out = refs[:5], refs[5:13], refs[13]
    grads = sources[4]
    views = [*sources[:4], grads.at[pl.ds(0, 3)], grads.at[3], grads.at[pl.ds(4, 2)], grads.at[6]]
    copies = [pltpu.make_async_copy(v, o, out.at[i]) for i, (v, o) in enumerate(zip(views, outs))]
    for copy in copies:
        copy.start()
    for copy in copies:
        copy.wait()


def shards(sizes, node_lat, edge_lat, receiver_row, sender_slot, send_rows, w_edge_in, w_edge_out, w_node_in,
           w_node_out, edge_gain, node_gain, node_cot, edge_cot):
    regions, feats = sizes
    per, width = node_lat.shape
    edges = edge_lat.shape[0]
    slots = send_rows.shape[2]
    part = width // feats // 2
    lines = (edges * feats // 128, 1, 128)
    scales = (1.0 / float(edges * feats * regions) ** 0.5, 1.0 / float(per * feats * regions) ** 0.5)
    ne, nn = EDGE_W[1], NODE_W[1]
    piece = ne * part // (regions // 2)

    def v(dtype, *shape):
        return pltpu.VMEM(shape, dtype)

    nodes_like = (feats, per, width)
    line_like = (regions, slots, width)

    def pair(dtype, *shape):
        return [v(dtype, *shape)] * 2

    scratch = [
        v(BF16, SIDE, SIDE, per, width), v(F32, feats, 1, 128), v(BF16, ne + nn, SIDE, SIDE, 2, part, width),
        *pair(BF16, *line_like),
        *pair(F32, edges, width),
        *[v(BF16, edges, width)] * 4,
        *pair(BF16, *nodes_like), v(BF16, *nodes_like), *pair(BF16, *nodes_like), *pair(BF16, *line_like),
        v(F32, ne + nn, feats, 2, part, width),
        *pair(BF16, ne, feats, part, width), *pair(BF16, nn, feats, part, width),
        *pair(BF16, SIDE, ne, SIDE, part, width), *pair(BF16, SIDE, nn, SIDE, part, width),
        *pair(BF16, SIDE, ne, part, width), *pair(BF16, SIDE, nn, part, width),
        *pair(BF16, regions // 2, piece, width), *pair(BF16, regions // 2, piece, width),
        *pair(BF16, regions, piece, width),
        pltpu.SemaphoreType.DMA((37,)), pltpu.SemaphoreType.DMA((37,)),
    ]

    args = (node_lat, edge_lat, receiver_row.reshape(lines), sender_slot.reshape(lines), send_rows,
            w_edge_in.reshape(3, 2, part, width), w_edge_out.reshape(2, part, width),
            w_node_in.reshape(2, 2, part, width), w_node_out.reshape(2, part, width),
            edge_gain[None], node_gain[None], node_cot, edge_cot)
    n = len(args)
    scratch += [*[v(x.dtype, *x.shape) for x in args], pltpu.SemaphoreType.DMA((n,))]

    def body(*refs):
        sources, rest = refs[:n], refs[n:]
        held, sem = rest[-n - 1:-1], rest[-1]
        fetches = [pltpu.make_async_copy(s, h, sem.at[i]) for i, (s, h) in enumerate(zip(sources, held))]
        for fetch in fetches:
            fetch.start()
        kernel(regions, feats, scales, fetches, *held, *rest[:-n - 1])

    vmem = pl.BlockSpec(memory_space=pltpu.VMEM)
    kinds = [((per, width), BF16), ((edges, width), BF16), ((per, width), F32), ((edges, width), F32)]
    blocks = [(3, 2, part, width), (2, part, width), (2, 2, part, width), (2, part, width)]
    results = pl.pallas_call(
        body,
        name="layer",
        out_shape=[jax.ShapeDtypeStruct(*k) for k in (*kinds, ((ne + nn, 2, part, width), F32))],
        in_specs=[pl.BlockSpec(memory_space=pltpu.HBM)] * n,
        out_specs=[vmem] * 5,
        scratch_shapes=scratch,
        compiler_params=pltpu.CompilerParams(
            collective_id=0, has_side_effects=True, vmem_limit_bytes=VMEM_LIMIT),
    )(*[pltpu.with_memory_space_constraint(x, pltpu.HBM) for x in args])
    kinds += [(s, F32) for s in blocks]
    outs = pl.pallas_call(
        hand_on,
        name="hand_on",
        out_shape=[jax.ShapeDtypeStruct(*k) for k in kinds],
        in_specs=[vmem] * 5,
        out_specs=[pl.BlockSpec(memory_space=pltpu.HBM)] * 8,
        scratch_shapes=[pltpu.SemaphoreType.DMA((8,))],
        compiler_params=pltpu.CompilerParams(vmem_limit_bytes=8 * 2**20),
    )(*results)
    return (*outs[:4], outs[4].reshape(3, 2 * part, width), outs[5].reshape(2 * part, width),
            outs[6].reshape(2, 2 * part, width), outs[7].reshape(2 * part, width))


def solution(mesh):
    rows = P(("region", "feat"), None)
    blocks = (P(None, "feat", None), P("feat", None), P(None, "feat", None), P("feat", None))
    in_specs = (rows, rows, P("region"), P("region"), P("region", None, None), *blocks, P("feat"), P("feat"), rows, rows)
    sizes = (mesh.shape["region"], mesh.shape["feat"])
    return jax.shard_map(lambda *args: shards(sizes, *args), mesh=mesh, in_specs=in_specs,
                         out_specs=(rows, rows, rows, rows, *blocks), check_vma=False)
```

```python
import jax
import jax.numpy as jnp
from jax import lax
from jax.experimental import pallas as pl
from jax.experimental.pallas import tpu as pltpu
from jax.sharding import PartitionSpec as P

MESH = pl.DeviceIdType.MESH
BF16, F32 = jnp.bfloat16, jnp.float32
EPSILON = 1e-05
SIDE = 4
EDGE_W, NODE_W = (0, 4), (4, 3)
VMEM_LIMIT = 44 * 2**20


def hops(d, n):
    return min(d, n - d)


def far_first(n):
    return sorted(range(1, n), key=lambda d: -hops(d, n))


PLANE_STEPS = sorted(((dy, dx) for dy in range(SIDE) for dx in range(SIDE) if dy or dx),
                     key=lambda s: -hops(s[0], SIDE) - hops(s[1], SIDE))


def dot(a, b, da, db):
    return lax.dot_general(a, b, (((da,), (db,)), ((), ())), preferred_element_type=F32)


def mm(a, b):
    return dot(a, b, 1, 0)


def mm_back(a, b):
    return dot(a, b, 1, 1)


def mm_t(a, b):
    return dot(a, b, 0, 0)


def sigmoid(v):
    return 1.0 / (1.0 + jnp.exp(-v))


def layer_norm(m):
    width = m.shape[1]
    mean = jnp.sum(m, axis=1, keepdims=True) / width
    var = jnp.sum(m * m, axis=1, keepdims=True) / width - mean * mean
    inverse = lax.rsqrt(var + EPSILON)
    return (m - mean) * inverse, inverse


def layer_norm_back(cot, normed, inverse, gain):
    width = cot.shape[1]
    s = cot * gain
    first = jnp.sum(s, axis=1, keepdims=True) / width
    second = jnp.sum(s * normed, axis=1, keepdims=True) / width
    return (inverse * (s - first - normed * second)).astype(BF16)


def iota(shape, dim):
    return lax.broadcasted_iota(jnp.int32, shape, dim)


def rows_equal(count, index, base=0):
    rows = iota((count, index.shape[1]), 0) + base
    return jnp.where(rows == index, 1.0, 0.0).astype(BF16)


def flat(blocks, pick, mine):
    wide = lax.dot_general(blocks, jnp.where(pick, 1.0, 0.0), (((1,), (0,)), ((), ())),
                           precision=lax.Precision.HIGHEST, preferred_element_type=F32)
    return jnp.sum(jnp.where(mine, wide, 0.0), axis=0, keepdims=True)


def own_slice(ref, f, edges):
    lines = 2 * edges // 128
    start = lax.div(f, 2) * lines
    two = jnp.concatenate([ref[start + i] for i in range(lines)], axis=1)
    return jnp.where(lax.rem(f, 2) == 1, two[:, edges:], two[:, :edges])


def kernel(regions, feats, scales, fetches,
           node, edge, recv_all, send_all, listed_at, wei, weo, wni, wno, egain, ngain, ncot, ecot,
           node_new, edge_new, node_grad, edge_grad, wgrad,
           nodes, gains, w, outgo, income, pre, normed, srows, rrows, hid, emg,
           pool_s, pool_r, npg, ng_s, ng_r, rem_s, rem_r,
           dw, pe_s, pe_r, pn_s, pn_r, re_s, re_r, rn_s, rn_r, qe_s, qe_r, qn_s, qn_r,
           ze_s, ze_r, zn_s, zn_r, be, bn, ssem, rsem):
    g, f = lax.axis_index("region"), lax.axis_index("feat")
    c, z = lax.rem(g, 2), lax.div(g, 2)
    y, x = lax.div(f, SIDE), lax.rem(f, SIDE)
    sibling = g + 1 - 2 * c
    first = c == 0
    a = jnp.where(first, x, y)
    b = jnp.where(first, y, x)
    chips = regions // 2
    per, width = node.shape
    edges = edge.shape[0]
    count = per * feats
    slots = income.shape[1]
    far = regions * slots

    def feat_at(a_, b_):
        return jnp.where(first, SIDE * b_ + a_, SIDE * a_ + b_)

    def send(src, dst, k, region, feat):
        return pltpu.make_async_remote_copy(
            src_ref=src, dst_ref=dst, send_sem=ssem.at[k], recv_sem=rsem.at[k],
            device_id=(region, feat), device_id_type=MESH)

    def to_plane(src_of, dst, k):
        for dy, dx in PLANE_STEPS:
            t = SIDE * lax.rem(y + dy, SIDE) + lax.rem(x + dx, SIDE)
            send(src_of(t), dst.at[f], k, g, t).start()

    def to_line(src_of, dst, k):
        for j in far_first(regions):
            t = lax.rem(g + j, regions)
            send(src_of(t), dst.at[g], k, t, f).start()

    def settle(view, k):
        send(view, view, k, g, f).wait()

    def settle_slots(buffer, k):
        settle(buffer.at[pl.ds(0, buffer.shape[0] - 1)], k)

    barrier = pltpu.get_barrier_semaphore()

    for (dy, dx), j in zip(PLANE_STEPS, far_first(regions)):
        t = SIDE * lax.rem(y + dy, SIDE) + lax.rem(x + dx, SIDE)
        pl.semaphore_signal(barrier, inc=1, device_id=(g, t), device_id_type=MESH)
        pl.semaphore_signal(barrier, inc=1, device_id=(lax.rem(g + j, regions), f), device_id_type=MESH)
    for fetch in fetches:
        fetch.wait()

    portion = egain.shape[1]
    gains[f] = jnp.concatenate([egain[...], ngain[...], jnp.zeros((1, gains.shape[2] - 2 * portion), F32)], axis=1)
    nodes[f] = node[...]
    for k in range(3):
        w[k, y, x, c] = wei[k, c]
    w[3, y, x, c] = weo[c]
    for k in range(2):
        w[4 + k, y, x, c] = wni[k, c]
    w[6, y, x, c] = wno[c]
    income[g] = jnp.zeros(income.shape[1:], BF16)
    rem_r[g] = jnp.zeros(rem_r.shape[1:], BF16)
    recv_at = own_slice(recv_all, f, edges)
    send_at = own_slice(send_all, f, edges)
    grid = (regions, far)
    listed = flat(listed_at[0].astype(F32), lax.rem(iota((slots, far), 1), slots) == iota((slots, far), 0),
                  lax.div(iota(grid, 1), slots) == iota(grid, 0))
    asked = jnp.where(iota((count, far), 0).astype(F32) == listed, 1.0, 0.0).astype(BF16)
    into = rows_equal(count, recv_at)
    near = rows_equal(count, send_at)
    away = rows_equal(far, send_at, count)
    pl.semaphore_wait(barrier, feats - 1 + regions - 1)

    def weights_first(group, k):
        part = w.at[pl.ds(*group), y, x, c]
        for d in (2, 1, 3):
            send(part, part, k, g, feat_at(lax.rem(a + d, SIDE), b)).start()

    def bundle(group, b_, act):
        ks = pl.ds(*group)

        @pl.when(first)
        def _():
            act(w.at[ks, b_, :, 0])

        @pl.when(c == 1)
        def _():
            act(w.at[ks, :, b_, 1])

    def weights_second(group, k, k2):
        settle(w.at[pl.ds(*group), 0, pl.ds(0, SIDE - 1), 0], k)

        def act(part):
            for d in (2, 1, 3):
                send(part, part, k2 + d, g, feat_at(a, lax.rem(b + d, SIDE))).start()
            send(part, part, k2, sibling, f).start()
        bundle(group, b, act)

    def weights_pass(group, k2, d):
        settle(w.at[pl.ds(*group), 0, :, 0], k2 + d)
        bundle(group, lax.rem(b - d + SIDE, SIDE), lambda part: send(part, part, k2, sibling, f).start())

    def weights_end(group, k2):
        settle(w.at[pl.ds(*group), :, :, 0], k2)

    weights_first(EDGE_W, 2)
    to_plane(lambda t: node, nodes, 0)
    weights_first(NODE_W, 3)
    to_plane(lambda t: gains.at[f], gains, 1)
    weights_second(EDGE_W, 2, 5)
    settle_slots(nodes, 0)
    table = nodes[...].reshape(count, width)
    outgo[...] = mm_t(asked, table).astype(BF16).reshape(outgo.shape)
    to_line(lambda t: outgo.at[t], income, 4)
    weights_second(NODE_W, 3, 9)
    rrows[...] = mm_t(into, table).astype(BF16)
    near_rows = mm_t(near, table)
    settle_slots(gains, 1)
    packed = gains[...].reshape(feats, gains.shape[2])
    shape, wide = (gains.shape[2], 2 * width), (feats, 2 * width)
    lanes = iota(shape, 1)
    gain = flat(packed, lax.rem(lanes, portion) + portion * lax.div(lanes, width) == iota(shape, 0),
                lax.div(lax.rem(iota(wide, 1), width), portion) == iota(wide, 0))
    edge_gain, node_gain = gain[:, :width], gain[:, width:]
    weights_pass(EDGE_W, 5, 1)
    weights_pass(EDGE_W, 5, 3)
    weights_pass(EDGE_W, 5, 2)
    settle_slots(income, 4)
    srows[...] = (near_rows + mm_t(away, income[...].reshape(far, width))).astype(BF16)
    weights_end(EDGE_W, 5)

    def weight(k):
        return w[k].reshape(width, width)

    pre[...] = mm(edge[...], weight(0)) + mm(srows[...], weight(1)) + mm(rrows[...], weight(2))
    hid[...] = (pre[...] * sigmoid(pre[...])).astype(BF16)
    edge_normed, edge_inverse = layer_norm(mm(hid[...], weight(3)))
    normed[...] = edge_normed
    fresh = (edge[...].astype(F32) + edge_normed * edge_gain).astype(BF16)
    edge_new[...] = fresh
    pool_s[...] = mm(into, fresh).astype(BF16).reshape(pool_s.shape)
    pool_r[f] = pool_s[f]
    to_plane(lambda t: pool_s.at[t], pool_r, 13)
    for d in (1, 3, 2):
        weights_pass(NODE_W, 9, d)
    gate = sigmoid(pre[...])
    pre[...] = gate * (1.0 + pre[...] * (1.0 - gate))
    weights_end(NODE_W, 9)
    lat = node[...]
    node_base = mm(lat, weight(4))
    settle_slots(pool_r, 13)

    pooled = jnp.sum(pool_r[...].astype(F32), axis=0).astype(BF16)
    node_pre = node_base + mm(pooled, weight(5))
    gate = sigmoid(node_pre)
    node_hid = (node_pre * gate).astype(BF16)
    node_normed, node_inverse = layer_norm(mm(node_hid, weight(6)))
    node_new[...] = (lat.astype(F32) + node_normed * node_gain).astype(BF16)
    nmg = layer_norm_back(ncot[...].astype(F32), node_normed, node_inverse, node_gain)
    slope = gate * (1.0 + node_pre * (1.0 - gate))
    own_npg = (mm_back(nmg, weight(6)) * slope).astype(BF16)
    npg[f] = own_npg
    to_plane(lambda t: npg.at[f], npg, 14)

    def trade(k, product, out, back, s):
        dw[k] = product.reshape(dw.shape[1:])
        out[...] = dw[k, :, 1 - c].astype(BF16)
        send(out, back, s, sibling, f).start()

    def along_a(k, i, back, stage, landed, s, s2):
        settle(back, s)

        def body(j, carry):
            a_, b_ = lax.div(j, SIDE), lax.rem(j, SIDE)
            at = feat_at(a_, b_)
            stage[a_, i, b_] = (dw[k, at, c] + back[at].astype(F32)).astype(BF16)
            return carry
        lax.fori_loop(0, feats, body, 0, unroll=True)
        landed[a, i] = stage[a, i]
        for d in (2, 1, 3):
            a_ = lax.rem(a + d, SIDE)
            send(stage.at[a_, i], landed.at[a, i], s2, g, feat_at(a_, b)).start()

    def along_b(landed, stage, landed2, k2, k3):
        settle_slots(landed, k2)

        def body(b_, carry):
            stage[b_] = jnp.sum(landed[:, :, b_].astype(F32), axis=0).astype(BF16)
            return carry
        lax.fori_loop(0, SIDE, body, 0)
        landed2[b] = stage[b]
        for d in (2, 1, 3):
            b_ = lax.rem(b + d, SIDE)
            send(stage.at[b_], landed2.at[b], k3, g, feat_at(a, b_)).start()

    def along_z(landed, stage, landed2, k3, k4):
        settle_slots(landed, k3)
        whole = jnp.sum(landed[...].astype(F32), axis=0).astype(BF16)
        rows = stage.shape[1]
        pieces = whole.reshape(whole.shape[0] * whole.shape[1] // rows, rows, width)
        stage[pl.ds(0, pieces.shape[0])] = pieces
        if pieces.shape[0] < chips:
            stage[pl.ds(pieces.shape[0], chips - pieces.shape[0])] = jnp.zeros(
                (chips - pieces.shape[0], rows, width), BF16)
        landed2[z] = stage[z]
        for d in far_first(chips):
            z_ = lax.rem(z + d, chips)
            send(stage.at[z_], landed2.at[z], k4, 2 * z_ + c, f).start()

    def to_all(landed, whole, k4, k5, scale):
        settle_slots(landed, k4)
        whole[g] = (jnp.sum(landed[...].astype(F32), axis=0) * scale).astype(BF16)
        to_line(lambda t: whole.at[g], whole, k5)

    def finish(group, whole, k5):
        settle_slots(whole, k5)
        start, n = group
        rows = whole.shape[1]
        halves = wgrad.shape[2] // rows
        for i in range(n):
            for c_ in range(2):
                for h in range(halves):
                    wgrad[start + i, c_, pl.ds(h * rows, rows)] = whole[2 * (halves * i + h) + c_].astype(F32)

    node_sides = ((lat, own_npg), (pooled, own_npg), (node_hid, nmg))
    for i in range(3):
        trade(4 + i, mm_t(*node_sides[i]), pn_s.at[i], pn_r.at[i], 29 + i)
    direct = ncot[...].astype(F32) + mm_back(own_npg, weight(4))
    for i in range(3):
        along_a(4 + i, i, pn_r.at[i], rn_s, rn_r, 29 + i, 16)
    settle_slots(npg, 14)

    reached = mm_t(into, npg[...].reshape(count, width)).astype(BF16)
    total = ecot[...].astype(F32) + mm_back(reached, weight(5))
    emg[...] = layer_norm_back(total, normed[...], edge_inverse, edge_gain)
    pre_grad = (mm_back(emg[...], weight(3)) * pre[...]).astype(BF16)
    trade(3, mm_t(hid[...], emg[...]), pe_s.at[3], pe_r.at[3], 35)
    from_send = mm_back(pre_grad, weight(1)).astype(BF16)
    rem_s[...] = mm(away, from_send).astype(BF16).reshape(rem_s.shape)
    to_line(lambda t: rem_s.at[t], rem_r, 18)
    trade(0, mm_t(edge[...], pre_grad), pe_s.at[0], pe_r.at[0], 32)
    along_a(3, 3, pe_r.at[3], re_s, re_r, 35, 19)
    trade(1, mm_t(srows[...], pre_grad), pe_s.at[1], pe_r.at[1], 33)
    along_a(0, 0, pe_r.at[0], re_s, re_r, 32, 19)
    trade(2, mm_t(rrows[...], pre_grad), pe_s.at[2], pe_r.at[2], 34)
    along_a(1, 1, pe_r.at[1], re_s, re_r, 33, 19)
    along_a(2, 2, pe_r.at[2], re_s, re_r, 34, 19)
    along_b(rn_r, qn_s, qn_r, 16, 20)
    from_recv = mm_back(pre_grad, weight(2)).astype(BF16)
    ng = mm(near, from_send) + mm(into, from_recv)
    edge_grad[...] = total + mm_back(pre_grad, weight(0))
    along_b(re_r, qe_s, qe_r, 19, 24)

    settle_slots(rem_r, 18)
    ng = ng + mm(asked, rem_r[...].reshape(far, width))
    ng_s[...] = ng.astype(BF16).reshape(ng_s.shape)
    ng_r[f] = ng_s[f]
    along_z(qn_r, zn_s, zn_r, 20, 23)
    along_z(qe_r, ze_s, ze_r, 24, 26)
    to_plane(lambda t: ng_s.at[t], ng_r, 21)
    to_all(zn_r, bn, 23, 27, scales[1])
    to_all(ze_r, be, 26, 28, scales[0])
    settle_slots(ng_r, 21)
    node_grad[...] = direct + jnp.sum(ng_r[...].astype(F32), axis=0)
    finish(NODE_W, bn, 27)
    finish(EDGE_W, be, 28)


def hand_on(*refs):
    sources, outs, out = refs[:5], refs[5:13], refs[13]
    grads = sources[4]
    views = [*sources[:4], grads.at[pl.ds(0, 3)], grads.at[3], grads.at[pl.ds(4, 2)], grads.at[6]]
    copies = [pltpu.make_async_copy(v, o, out.at[i]) for i, (v, o) in enumerate(zip(views, outs))]
    for copy in copies:
        copy.start()
    for copy in copies:
        copy.wait()


def shards(sizes, node_lat, edge_lat, receiver_row, sender_slot, send_rows, w_edge_in, w_edge_out, w_node_in,
           w_node_out, edge_gain, node_gain, node_cot, edge_cot):
    regions, feats = sizes
    per, width = node_lat.shape
    edges = edge_lat.shape[0]
    slots = send_rows.shape[2]
    part = width // feats // 2
    lines = (edges * feats // 128, 1, 128)
    scales = (1.0 / float(edges * feats * regions) ** 0.5, 1.0 / float(per * feats * regions) ** 0.5)
    ne, nn = EDGE_W[1], NODE_W[1]
    piece = ne * part // (regions // 2)

    def v(dtype, *shape):
        return pltpu.VMEM(shape, dtype)

    nodes_like = (feats, per, width)
    line_like = (regions, slots, width)

    def pair(dtype, *shape):
        return [v(dtype, *shape)] * 2

    scratch = [
        v(BF16, *nodes_like), v(F32, feats, 1, 128), v(BF16, ne + nn, SIDE, SIDE, 2, part, width),
        *pair(BF16, *line_like),
        *pair(F32, edges, width),
        *[v(BF16, edges, width)] * 4,
        *pair(BF16, *nodes_like), v(BF16, *nodes_like), *pair(BF16, *nodes_like), *pair(BF16, *line_like),
        v(F32, ne + nn, feats, 2, part, width),
        *pair(BF16, ne, feats, part, width), *pair(BF16, nn, feats, part, width),
        *pair(BF16, SIDE, ne, SIDE, part, width), *pair(BF16, SIDE, nn, SIDE, part, width),
        *pair(BF16, SIDE, ne, part, width), *pair(BF16, SIDE, nn, part, width),
        *pair(BF16, regions // 2, piece, width), *pair(BF16, regions // 2, piece, width),
        *pair(BF16, regions, piece, width),
        pltpu.SemaphoreType.DMA((36,)), pltpu.SemaphoreType.DMA((36,)),
    ]

    args = (node_lat, edge_lat, receiver_row.reshape(lines), sender_slot.reshape(lines), send_rows,
            w_edge_in.reshape(3, 2, part, width), w_edge_out.reshape(2, part, width),
            w_node_in.reshape(2, 2, part, width), w_node_out.reshape(2, part, width),
            edge_gain[None], node_gain[None], node_cot, edge_cot)
    n = len(args)
    scratch += [*[v(x.dtype, *x.shape) for x in args], pltpu.SemaphoreType.DMA((n,))]

    def body(*refs):
        sources, rest = refs[:n], refs[n:]
        held, sem = rest[-n - 1:-1], rest[-1]
        fetches = [pltpu.make_async_copy(s, h, sem.at[i]) for i, (s, h) in enumerate(zip(sources, held))]
        for fetch in fetches:
            fetch.start()
        kernel(regions, feats, scales, fetches, *held, *rest[:-n - 1])

    vmem = pl.BlockSpec(memory_space=pltpu.VMEM)
    kinds = [((per, width), BF16), ((edges, width), BF16), ((per, width), F32), ((edges, width), F32)]
    blocks = [(3, 2, part, width), (2, part, width), (2, 2, part, width), (2, part, width)]
    results = pl.pallas_call(
        body,
        name="layer",
        out_shape=[jax.ShapeDtypeStruct(*k) for k in (*kinds, ((ne + nn, 2, part, width), F32))],
        in_specs=[pl.BlockSpec(memory_space=pltpu.HBM)] * n,
        out_specs=[vmem] * 5,
        scratch_shapes=scratch,
        compiler_params=pltpu.CompilerParams(
            collective_id=0, has_side_effects=True, vmem_limit_bytes=VMEM_LIMIT),
    )(*[pltpu.with_memory_space_constraint(x, pltpu.HBM) for x in args])
    kinds += [(s, F32) for s in blocks]
    outs = pl.pallas_call(
        hand_on,
        name="hand_on",
        out_shape=[jax.ShapeDtypeStruct(*k) for k in kinds],
        in_specs=[vmem] * 5,
        out_specs=[pl.BlockSpec(memory_space=pltpu.HBM)] * 8,
        scratch_shapes=[pltpu.SemaphoreType.DMA((8,))],
        compiler_params=pltpu.CompilerParams(vmem_limit_bytes=8 * 2**20),
    )(*results)
    return (*outs[:4], outs[4].reshape(3, 2 * part, width), outs[5].reshape(2 * part, width),
            outs[6].reshape(2, 2 * part, width), outs[7].reshape(2 * part, width))


def solution(mesh):
    rows = P(("region", "feat"), None)
    blocks = (P(None, "feat", None), P("feat", None), P(None, "feat", None), P("feat", None))
    in_specs = (rows, rows, P("region"), P("region"), P("region", None, None), *blocks, P("feat"), P("feat"), rows, rows)
    sizes = (mesh.shape["region"], mesh.shape["feat"])
    return jax.shard_map(lambda *args: shards(sizes, *args), mesh=mesh, in_specs=in_specs,
                         out_specs=(rows, rows, rows, rows, *blocks), check_vma=False)
```
